32 devices in a mesh: row: 4 (over y, core), col: 8 (over z, x).
Axes of the slice: x: 2, y: 2, z: 4, core: 2. Of those that a mesh axis runs over, the one named last changes fastest.
Arguments:
- u_state: float32 [2048, 128], P(('row', 'col')), may hold values from -12 to 12
- v_state: float32 [3, 2048, 128], P(None, ('col', 'row')), may hold values from -12 to 12
- alpha_prev: float32 [128], replicated, may hold values from 0.5 to 2
- near_blocks: bfloat16 [4, 8, 16, 128, 3, 128], P('row', 'col'), may hold values from -0.3125 to 0.3125
- near_rows: int32 [4, 8, 16], P('row', 'col'), may hold values from 0 to 3
- near_cols: int32 [4, 8, 16], P('row', 'col'), may hold values from 0 to 1
- near_count: int32 [4, 8], P('row', 'col'), may hold values from 4 to 16, as said below
- mid_left: bfloat16 [8, 64, 2048], P('col', None, 'row'), may hold values from -0.75 to 0.75
- mid_right: bfloat16 [4, 64, 3, 2048], P('row', None, None, 'col'), may hold values from -0.21875 to 0.21875
- mid_rank: int32 [4, 8], P('row', 'col'), may hold values from 32 to 64
- coarse_left: bfloat16 [8, 32, 2048], P('col', None, 'row'), may hold values from -1 to 1
- coarse_right: bfloat16 [32, 3, 2048], P(None, None, ('col', 'row')), may hold values from -0.21875 to 0.21875
- coarse_rank: int32 [8], P('col'), may hold values from 16 to 32
Outputs:
- u_next: float32 [2048, 128], P(('row', 'col'))
- v_next: float32 [3, 2048, 128], P(None, ('col', 'row'))
- norms: float32 [2, 128], replicated
The draws below stay inside these ranges and needn't reach their ends.
Inputs may be any that keep to these rules, and one draw needn't show every extreme that they name: Slots 0 to near_count - 1 of a block are live; some block has all 16 slots live.
All inputs are finite; a program needn't handle non-finite values.
Results may differ from the reference program's by a relative error of at most 0.0044.
Values may be sent and summed in bfloat16 or wider, within the bound.
A program may use at most 64 MiB of HBM per device.

```python
import jax
import jax.numpy as jnp
from jax import lax

PT_DEV = 64
PAT_DEV = 64
RHS = 128
NEAR = 16
CLP = 128
CLQ = 128
RANK_MID = 64
RANK_COARSE = 32
ROW_CLUSTERS = 4
COL_CLUSTERS = 2
POINTS = 2048
PATCHES = 2048
N_ROW = 4
N_COL = 8


def draw_u_state(key, part):
    ramp = 1.0 + 2.0 * jnp.arange(POINTS, dtype=jnp.float32) / POINTS
    base = jnp.clip(jax.random.normal(key, (POINTS, RHS), jnp.float32), -4.0, 4.0)
    return (base * ramp[:, None]).astype(jnp.float32)


def draw_v_state(key, part):
    ramp = 1.0 + 2.0 * jnp.arange(PATCHES, dtype=jnp.float32) / PATCHES
    base = jnp.clip(jax.random.normal(key, (3, PATCHES, RHS), jnp.float32), -4.0, 4.0)
    return (base * ramp[None, :, None]).astype(jnp.float32)


def draw_near_count(key, part):
    divisor = jax.random.randint(key, (N_ROW, N_COL), 1, 5)
    counts = jnp.maximum(NEAR // divisor, 1)
    chosen = jax.random.randint(jax.random.fold_in(key, 11), (), 0, N_ROW * N_COL)
    counts = counts.reshape(-1).at[chosen].set(NEAR).reshape(N_ROW, N_COL)
    return counts.astype(jnp.int32)


def set_ends(values, key, least, top_value):
    dims = values.shape
    spot = [jax.random.randint(jax.random.fold_in(key, axis), (), 0, dims[axis]) for axis in range(len(dims))]
    values = values.at[tuple(spot)].set(least)
    longest = dims.index(max(dims))
    spot[longest] = (spot[longest] + 1) % dims[longest]
    return values.at[tuple(spot)].set(top_value)


def shard_levels(stream_key, extent, pieces, least, high):
    gain, own = 1.0, jax.random.fold_in(stream_key, 6)
    for dim, parts in pieces:
        draws = jnp.exp(jax.random.uniform(jax.random.fold_in(own, dim), (parts,), jnp.float32, least / len(pieces), high / len(pieces)))
        gain = gain * jnp.repeat(draws, extent[dim] // parts).reshape([-1 if axis == dim else 1 for axis in range(len(extent))])
    return gain


def scatter_about(own_key, shape, spread, most, shards=(), kind=jnp.bfloat16):
    gain = shard_levels(own_key, shape, shards, -0.22, 0.18) if shards else 1.0
    drawn = jax.random.normal(own_key, shape, jnp.float32) * spread * gain
    return jnp.minimum(jnp.maximum(drawn, -most), most).astype(kind)


def setup_inputs(seed: int = 0) -> dict:
    arg_keys = jax.random.split(jax.random.key(seed), 14)
    return {
        "u_state": draw_u_state(jax.random.fold_in(arg_keys[13], 71), 0),
        "v_state": draw_v_state(jax.random.fold_in(arg_keys[13], 71), 0),
        "alpha_prev": jnp.clip(jax.random.uniform(arg_keys[2], (RHS,), jnp.float32, 0.5, 2.0), 0.5, 2.0),
        "near_blocks": scatter_about(arg_keys[3], (N_ROW, N_COL, NEAR, CLP, 3, CLQ), (3 * CLQ) ** -0.5, 0.3125, ((0, 4), (1, 8))),
        "near_rows": set_ends(jax.random.randint(arg_keys[4], (N_ROW, N_COL, NEAR), 0, ROW_CLUSTERS), jax.random.fold_in(arg_keys[4], 1), 0, ROW_CLUSTERS - 1).astype(jnp.int32),
        "near_cols": set_ends(jax.random.randint(arg_keys[5], (N_ROW, N_COL, NEAR), 0, COL_CLUSTERS), jax.random.fold_in(arg_keys[5], 1), 0, COL_CLUSTERS - 1).astype(jnp.int32),
        "near_count": draw_near_count(jax.random.fold_in(arg_keys[13], 71), 0),
        "mid_left": scatter_about(arg_keys[7], (N_COL, RANK_MID, POINTS), RANK_MID ** -0.5, 0.75, ((0, 8), (2, 4))),
        "mid_right": scatter_about(arg_keys[8], (N_ROW, RANK_MID, 3, PATCHES), (3 * PAT_DEV * N_ROW) ** -0.5, 0.21875, ((0, 4), (3, 8))),
        "mid_rank": set_ends(jax.random.randint(arg_keys[9], (N_ROW, N_COL), RANK_MID // 2, RANK_MID + 1), jax.random.fold_in(arg_keys[9], 1), RANK_MID // 2, RANK_MID).astype(jnp.int32),
        "coarse_left": scatter_about(arg_keys[10], (N_COL, RANK_COARSE, POINTS), RANK_COARSE ** -0.5, 1.0, ((0, 8), (2, 4))),
        "coarse_right": scatter_about(arg_keys[11], (RANK_COARSE, 3, PATCHES), (3 * PAT_DEV * N_ROW) ** -0.5, 0.21875, ((2, 32),)),
        "coarse_rank": set_ends(jax.random.randint(arg_keys[12], (N_COL,), RANK_COARSE // 2, RANK_COARSE + 1), jax.random.fold_in(arg_keys[12], 1), RANK_COARSE // 2, RANK_COARSE).astype(jnp.int32),
    }


tiny_add = 1e-06

def reference(u_state, v_state, alpha_prev, near_blocks, near_rows, near_cols, near_count, mid_left, mid_right, mid_rank, coarse_left, coarse_right, coarse_rank):
    row_span = PT_DEV * N_COL
    col_span = PAT_DEV * N_ROW
    row_groups = row_span // CLP
    col_groups = col_span // CLQ
    devices_all = N_ROW * N_COL
    slip_half = v_state.astype(jnp.bfloat16)
    slip_cols = slip_half.reshape(3, N_COL, col_span, RHS).transpose(1, 0, 2, 3)
    right_cols = coarse_right.reshape(RANK_COARSE, 3, N_COL, col_span).astype(jnp.float32)
    coarse_keep = (jnp.arange(RANK_COARSE)[None, :] < coarse_rank[:, None]).astype(jnp.float32)
    coarse_codes = jnp.einsum('kcjp,jcps->jks', right_cols, slip_cols.astype(jnp.float32))
    coarse_codes = (coarse_codes * coarse_keep[:, :, None]).astype(jnp.bfloat16)
    blocks_all = near_blocks.reshape(devices_all, NEAR, CLP, 3, CLQ)
    rows_all = near_rows.reshape(devices_all, NEAR)
    cols_all = near_cols.reshape(devices_all, NEAR)
    count_all = near_count.reshape(devices_all)
    left_mid_all = mid_left.reshape(N_COL, RANK_MID, N_ROW, row_span).transpose(2, 0, 1, 3).reshape(devices_all, RANK_MID, row_span)
    right_mid_all = mid_right.reshape(N_ROW, RANK_MID, 3, N_COL, col_span).transpose(0, 3, 1, 2, 4).reshape(devices_all, RANK_MID, 3, col_span)
    rank_all = mid_rank.reshape(devices_all)
    left_coarse_all = coarse_left.reshape(N_COL, RANK_COARSE, N_ROW, row_span).transpose(2, 0, 1, 3).reshape(devices_all, RANK_COARSE, row_span)
    device_ids = jnp.arange(devices_all, dtype=jnp.int32)
    inputs_all = (device_ids, blocks_all, rows_all, cols_all, count_all, left_mid_all, right_mid_all, rank_all, left_coarse_all)

    def forward_step(total, items):
        device_id, blocks, rows_index, cols_index, live_count, left_mid, right_mid, rank_mid, left_coarse = items
        row_id = device_id // N_COL
        col_id = device_id % N_COL
        slip_col = slip_cols[col_id]
        segments = jnp.take(slip_col.reshape(3, col_groups, CLQ, RHS), cols_index, axis=1)
        products = jnp.einsum('npkq,knqs->nps', blocks.astype(jnp.float32), segments.astype(jnp.float32))
        live_mask = (jnp.arange(NEAR) < live_count).astype(jnp.float32)
        products = products * live_mask[:, None, None]
        near_part = jnp.zeros((row_groups, CLP, RHS), jnp.float32).at[rows_index].add(products).reshape(row_span, RHS)
        mid_keep = (jnp.arange(RANK_MID) < rank_mid).astype(jnp.float32)[:, None]
        mid_codes = jnp.einsum('kcp,cps->ks', right_mid.astype(jnp.float32), slip_col.astype(jnp.float32))
        mid_codes = (mid_codes * mid_keep).astype(jnp.bfloat16)
        mid_part = jnp.einsum('kr,ks->rs', left_mid.astype(jnp.float32), mid_codes.astype(jnp.float32))
        coarse_part = jnp.einsum('kr,ks->rs', left_coarse.astype(jnp.float32), coarse_codes[col_id].astype(jnp.float32))
        total = total.at[row_id].add(near_part + mid_part + coarse_part)
        return (total, None)
    rows_total, _ = lax.scan(forward_step, jnp.zeros((N_ROW, row_span, RHS), jnp.float32), inputs_all)
    u_hat = rows_total.reshape(N_ROW * row_span, RHS) - alpha_prev[None, :] * u_state
    beta_new = jnp.sqrt(lax.optimization_barrier(jnp.mean(u_hat * u_hat, axis=0)) + tiny_add)
    u_next = u_hat / beta_new[None, :]
    resid_half = u_next.astype(jnp.bfloat16).reshape(N_ROW, row_span, RHS)

    def backward_step(carry, items):
        slip_total, coarse_sum = carry
        device_id, blocks, rows_index, cols_index, live_count, left_mid, right_mid, rank_mid, left_coarse = items
        row_id = device_id // N_COL
        col_id = device_id % N_COL
        resid_row = resid_half[row_id]
        row_segments = jnp.take(resid_row.reshape(row_groups, CLP, RHS), rows_index, axis=0)
        products = jnp.einsum('npkq,nps->knqs', blocks.astype(jnp.float32), row_segments.astype(jnp.float32))
        live_mask = (jnp.arange(NEAR) < live_count).astype(jnp.float32)
        products = products * live_mask[None, :, None, None]
        near_back = jnp.zeros((3, col_groups, CLQ, RHS), jnp.float32).at[:, cols_index].add(products).reshape(3, col_span, RHS)
        mid_keep = (jnp.arange(RANK_MID) < rank_mid).astype(jnp.float32)[:, None]
        mid_weights = jnp.einsum('kr,rs->ks', left_mid.astype(jnp.float32), resid_row.astype(jnp.float32))
        mid_weights = (mid_weights * mid_keep).astype(jnp.bfloat16)
        mid_back = jnp.einsum('kcp,ks->cps', right_mid.astype(jnp.float32), mid_weights.astype(jnp.float32))
        coarse_weights = jnp.einsum('kr,rs->ks', left_coarse.astype(jnp.float32), resid_row.astype(jnp.float32))
        coarse_weights = coarse_weights * coarse_keep[col_id][:, None]
        slip_total = slip_total.at[col_id].add(near_back + mid_back)
        coarse_sum = coarse_sum.at[col_id].add(coarse_weights)
        return ((slip_total, coarse_sum), None)
    start_carry = (jnp.zeros((N_COL, 3, col_span, RHS), jnp.float32), jnp.zeros((N_COL, RANK_COARSE, RHS), jnp.float32))
    (slip_total, coarse_sum), _ = lax.scan(backward_step, start_carry, inputs_all)
    backward = slip_total.transpose(1, 0, 2, 3).reshape(3, N_COL * col_span, RHS)
    coarse_back = jnp.einsum('kcjp,jks->cjps', right_cols, coarse_sum, precision=lax.Precision.HIGHEST)
    backward = backward + coarse_back.reshape(3, N_COL * col_span, RHS)
    v_hat = backward - beta_new[None, None, :] * v_state
    alpha_next = jnp.sqrt(lax.optimization_barrier(jnp.mean(v_hat * v_hat, axis=(0, 1))) + tiny_add)
    v_next = v_hat / alpha_next[None, None, :]
    return (u_next, v_next, jnp.stack([beta_new, alpha_next]))
```

```python
import functools

import jax
import jax.numpy as jnp
from jax import lax
from jax.experimental import pallas as pl
from jax.experimental.pallas import tpu as pltpu
from jax.sharding import PartitionSpec as P

tiny_add = 1e-06
MESH = pl.DeviceIdType.MESH
f32, bf16 = jnp.float32, jnp.bfloat16
WHOLE_LIMIT = 64


def fold(values):
    return (values * values).reshape(values.shape[0] // 8, 8, values.shape[1]).sum(axis=0)


def turn(values):
    return jnp.transpose(values.astype(f32), (1, 0))


def kernel(
    sizes,
    rows_hbm,
    cols_hbm,
    count_hbm,
    mid_rank_hbm,
    coarse_rank_hbm,
    u_hbm,
    v_hbm,
    alpha_hbm,
    near_hbm,
    mid_left_hbm,
    mid_right_hbm,
    coarse_left_hbm,
    coarse_right_hbm,
    u_out,
    v_out,
    beta_out,
    vsq_all,
    rows_smem,
    cols_smem,
    count_smem,
    mid_rank_smem,
    coarse_rank_smem,
    near,
    u_old,
    v_old,
    alpha_old,
    left,
    left_turned,
    right,
    slip,
    coarse_all,
    acc,
    fsend,
    frecv,
    ug,
    ut,
    sq,
    back_acc,
    bsend,
    brecv,
    vsq_col,
    near_sem,
    in_sem,
    slip_send,
    slip_recv,
    coarse_send,
    coarse_recv,
    f_send,
    f_recv,
    u_send,
    u_recv,
    sq_send,
    sq_recv,
    b_send,
    b_recv,
    vc_send,
    vc_recv,
    vr_send,
    vr_recv,
):
    n_row, n_col, unroll = sizes
    me_r, me_c = lax.axis_index("row"), lax.axis_index("col")
    slots, _, clp, clq = near.shape
    pt, rhs = u_old.shape
    pd = v_old.shape[1]
    km, kc = mid_left_hbm.shape[0], coarse_left_hbm.shape[0]
    kt = km + 2 * kc
    row_groups, col_groups = acc.shape[0], back_acc.shape[0]
    per_row, per_col = clp // pt, clq // pd

    def row_peer(step):
        return lax.rem(me_r + step, n_row)

    def far_first(me, count, step):
        upper = me >= count // 2
        own = jnp.where(upper, me, count - 1 - me)
        place = step - 1 + (step - 1 >= own).astype(jnp.int32)
        return jnp.where(upper, place, count - 1 - place)

    def col_peer(step):
        return far_first(me_c, n_col, step)

    loads = [
        pltpu.make_async_copy(src, dst, in_sem.at[place])
        for place, (src, dst) in enumerate(
            [
                (v_hbm, v_old),
                (coarse_right_hbm, coarse_all.at[me_r]),
                (mid_right_hbm, right.at[:, 0:km, :]),
                (mid_left_hbm, left.at[0:km, :]),
                (coarse_left_hbm, left.at[km : km + kc, :]),
                (coarse_left_hbm, left.at[km + kc : kt, :]),
                (u_hbm, u_old),
                (alpha_hbm, alpha_old),
                (rows_hbm, rows_smem),
                (cols_hbm, cols_smem),
                (count_hbm, count_smem),
                (mid_rank_hbm, mid_rank_smem),
                (coarse_rank_hbm, coarse_rank_smem),
            ]
        )
    ]
    loads[0].start()
    loads[1].start()

    barrier = pltpu.get_barrier_semaphore()
    whole = n_row * n_col <= WHOLE_LIMIT
    if whole:
        others = [(a, b) for b in range(n_col) for a in range(n_row)][1:]
        spots = [(lax.rem(me_r + a, n_row), lax.rem(me_c + b, n_col)) for a, b in others]
        for row, col in spots:
            pl.semaphore_signal(barrier, device_id=(row, col), device_id_type=MESH)
    else:
        spots = [(row_peer(step), me_c) for step in range(1, n_row)]
        spots += [(me_r, col_peer(step)) for step in range(1, n_col)]
        for row, col in spots:
            pl.semaphore_signal(barrier, device_id=(row, col), device_id_type=MESH)
    for load in loads[2:]:
        load.start()

    def near_load(slot):
        return pltpu.make_async_copy(near_hbm.at[slot], near.at[slot], near_sem.at[slot])

    def exchange(axis, me, count, peer, source, target, send_sem, recv_sem):
        copies = [
            pltpu.make_async_remote_copy(
                src_ref=source(peer(step)),
                dst_ref=target,
                send_sem=send_sem.at[step - 1],
                recv_sem=recv_sem.at[me],
                device_id={axis: peer(step)},
                device_id_type=MESH,
            )
            for step in range(1, count)
        ]
        for copy in copies:
            copy.start()
        incoming = [
            pltpu.make_async_remote_copy(
                src_ref=source(peer(step)),
                dst_ref=target,
                send_sem=send_sem.at[step - 1],
                recv_sem=recv_sem.at[peer(step)],
                device_id={axis: peer(step)},
                device_id_type=MESH,
            )
            for step in range(1, count)
        ]
        return copies, incoming

    def across_rows(source, target, send_sem, recv_sem):
        return exchange("row", me_r, n_row, row_peer, source, target, send_sem, recv_sem)

    def across_cols(source, target, send_sem, recv_sem):
        return exchange("col", me_c, n_col, col_peer, source, target, send_sem, recv_sem)

    def arrived(copies):
        for copy in copies[1]:
            copy.wait_recv()

    loads[0].wait()
    slip[me_r] = v_old[...].astype(bf16)
    loads[1].wait()
    pl.semaphore_wait(barrier, len(spots))
    sent_slip = across_rows(lambda peer: slip.at[me_r], slip.at[me_r], slip_send, slip_recv)
    sent_coarse = across_rows(
        lambda peer: coarse_all.at[me_r], coarse_all.at[me_r], coarse_send, coarse_recv
    )
    for slot in range(slots):
        near_load(slot).start()
    for load in loads[2:]:
        load.wait()
    for group in range(row_groups):
        span = slice(group * clp, (group + 1) * clp)
        left_turned[span, :] = turn(left[:, span]).astype(bf16)
    acc[...] = jnp.zeros_like(acc)
    back_acc[...] = jnp.zeros_like(back_acc)
    for slot in range(slots):
        near_load(slot).wait()
    arrived(sent_slip)

    def forward_steps(turn_index, carry):
        products, weights = [], []
        for inner in range(unroll):
            slot = turn_index * unroll + inner
            first = cols_smem[0, 0, slot] * per_col
            total = None
            for k in range(3):
                picked = slip[pl.ds(first, per_col), k].reshape(clq, rhs)
                term = jnp.dot(near[slot, k], picked, preferred_element_type=f32)
                total = term if total is None else total + term
            products.append(total)
            live = slot < count_smem[0, 0]
            weights.append(
                [
                    jnp.where(jnp.logical_and(rows_smem[0, 0, slot] == group, live), 1.0, 0.0).astype(f32)
                    for group in range(row_groups)
                ]
            )
        for group in range(row_groups):
            value = acc[group]
            for inner in range(unroll):
                value = value + products[inner] * weights[inner][group]
            acc[group] = value
        return carry

    lax.fori_loop(0, slots // unroll, forward_steps, 0)

    arrived(sent_coarse)
    for peer in range(n_row):
        for k in range(3):
            piece = coarse_all[peer, k]
            right[k, km : km + kc, peer * pd : (peer + 1) * pd] = piece
            right[k, km + kc : kt, peer * pd : (peer + 1) * pd] = piece
    codes = jnp.zeros((kt, rhs), f32)
    for k in range(3):
        codes = codes + jnp.dot(
            right[k], slip[:, k].reshape(n_row * pd, rhs), preferred_element_type=f32
        )
    place = lax.broadcasted_iota(jnp.int32, (kt, rhs), 0)
    limit = jnp.where(place < km, mid_rank_smem[0, 0], coarse_rank_smem[0])
    inside = jnp.where(place < km, place, jnp.where(place < km + kc, place - km, kt))
    codes = jnp.where(inside < limit, codes, 0.0).astype(bf16)
    for group in range(row_groups):
        span = slice(group * clp, (group + 1) * clp)
        value = acc[group] + jnp.dot(left_turned[span, :], codes, preferred_element_type=f32)
        fsend[group * per_row : (group + 1) * per_row] = value.astype(bf16).reshape(
            per_row, pt, rhs
        )
    sent_f = across_cols(lambda peer: fsend.at[peer], frecv.at[me_c], f_send, f_recv)
    frecv[me_c] = fsend[me_c]
    arrived(sent_f)
    u_hat = -alpha_old[...] * u_old[...]
    for peer in range(n_col):
        u_hat = u_hat + frecv[peer].astype(f32)
    ug[me_c] = u_hat.astype(bf16)
    sent_u = across_cols(lambda peer: ug.at[me_c], ug.at[me_c], u_send, u_recv)
    u_old[...] = u_hat
    arrived(sent_u)

    squares = jnp.zeros((8, rhs), f32)
    for group in range(row_groups):
        value = ug[group * per_row : (group + 1) * per_row].reshape(clp, rhs).astype(f32)
        squares = squares + fold(value)
        ut[group] = jnp.transpose(value, (1, 0)).astype(bf16)
    sq[me_r] = squares
    sent_sq = across_rows(lambda peer: sq.at[me_r], sq.at[me_r], sq_send, sq_recv)

    def backward_steps(turn_index, carry):
        products, weights = [], []
        for inner in range(unroll):
            slot = turn_index * unroll + inner
            picked = ut[rows_smem[0, 0, slot]]
            products.append(
                [jnp.dot(picked, near[slot, k], preferred_element_type=f32) for k in range(3)]
            )
            live = slot < count_smem[0, 0]
            weights.append(
                [
                    jnp.where(jnp.logical_and(cols_smem[0, 0, slot] == group, live), 1.0, 0.0).astype(f32)
                    for group in range(col_groups)
                ]
            )
        for group in range(col_groups):
            for k in range(3):
                value = back_acc[group, k]
                for inner in range(unroll):
                    value = value + products[inner][k] * weights[inner][group]
                back_acc[group, k] = value
        return carry

    lax.fori_loop(0, slots // unroll, backward_steps, 0)

    loads_turned = jnp.zeros((rhs, kt), f32)
    for group in range(row_groups):
        loads_turned = loads_turned + jnp.dot(
            ut[group],
            left_turned[group * clp : (group + 1) * clp, :],
            preferred_element_type=f32,
        )
    place = lax.broadcasted_iota(jnp.int32, (rhs, kt), 1)
    limit = jnp.where(place < km, mid_rank_smem[0, 0], coarse_rank_smem[0])
    inside = jnp.where(place < km, place, jnp.where(place < km + kc, place - km, place - km - kc))
    loads_turned = jnp.where(inside < limit, loads_turned, 0.0)
    high = loads_turned.astype(bf16)
    low = (loads_turned - high.astype(f32)).astype(bf16)
    factors = jnp.where(place < km + kc, high.astype(f32), low.astype(f32)).astype(bf16)
    for group in range(col_groups):
        for k in range(3):
            value = back_acc[group, k] + jnp.dot(
                factors,
                right[k, :, group * clq : (group + 1) * clq],
                preferred_element_type=f32,
            )
            value = jnp.transpose(value, (1, 0)).astype(bf16).reshape(per_col, pd, rhs)
            bsend[group * per_col : (group + 1) * per_col, k] = value
    sent_b = across_rows(lambda peer: bsend.at[peer], brecv.at[me_r], b_send, b_recv)
    brecv[me_r] = bsend[me_r]
    arrived(sent_sq)
    square_sum = jnp.zeros((8, rhs), f32)
    for peer in range(n_row):
        square_sum = square_sum + sq[peer]
    points = pt * n_row * n_col
    beta = jnp.sqrt(jnp.sum(square_sum, axis=0, keepdims=True) / points + tiny_add)
    beta_out[...] = beta
    u_out[...] = u_old[...] / beta
    arrived(sent_b)
    v_squares = jnp.zeros((8, rhs), f32)
    for k in range(3):
        total = jnp.zeros((pd, rhs), f32)
        for peer in range(n_row):
            total = total + brecv[peer, k].astype(f32)
        v_hat = total / beta - beta * v_old[k]
        v_out[k] = v_hat
        v_squares = v_squares + fold(v_hat)
    sent_v = []
    if whole:
        vsq_all[me_c, pl.ds(me_r, 1)] = jnp.sum(v_squares, axis=0, keepdims=True)

        def row_sum(place, row, col):
            return pltpu.make_async_remote_copy(
                src_ref=vsq_all.at[me_c, pl.ds(me_r, 1)],
                dst_ref=vsq_all.at[me_c, pl.ds(me_r, 1)],
                send_sem=vc_send.at[place],
                recv_sem=vc_recv.at[place],
                device_id=(row, col),
                device_id_type=MESH,
            )

        for place in reversed(range(len(spots))):
            copy = row_sum(place, *spots[place])
            copy.start()
            sent_v.append(copy)
        for copy in sent_v:
            copy.wait_recv()
    else:
        vsq_col[me_c] = v_squares
        sent_vc = across_cols(lambda peer: vsq_col.at[me_c], vsq_col.at[me_c], vc_send, vc_recv)
        arrived(sent_vc)
        v_squares = jnp.zeros((8, rhs), f32)
        for peer in range(n_col):
            v_squares = v_squares + vsq_col[peer]
        vsq_all[me_r] = v_squares
        sent_vr = across_rows(lambda peer: vsq_all.at[me_r], vsq_all.at[me_r], vr_send, vr_recv)
        arrived(sent_vr)
        sent_v = sent_vc[0] + sent_vr[0]
    for copies in (sent_slip, sent_coarse, sent_f, sent_u, sent_sq, sent_b):
        for copy in copies[0]:
            copy.wait_send()
    for copy in sent_v:
        copy.wait_send()


def finish(unknowns, u_ref, v_ref, beta_ref, squares_ref, u_out, v_out, norms_out):
    total = jnp.zeros(squares_ref.shape[1:], f32)
    for peer in range(squares_ref.shape[0]):
        total = total + squares_ref[peer]
    alpha = jnp.sqrt(jnp.sum(total, axis=0, keepdims=True) / unknowns + tiny_add)
    norms_out[0:1, :] = beta_ref[...]
    norms_out[1:2, :] = alpha
    u_out[...] = u_ref[...]
    v_out[...] = v_ref[...] / alpha


def per_device(
    n_row,
    n_col,
    u_state,
    v_state,
    alpha_prev,
    near_blocks,
    near_rows,
    near_cols,
    near_count,
    mid_left,
    mid_right,
    mid_rank,
    coarse_left,
    coarse_right,
    coarse_rank,
):
    slots, clp, _, clq = near_blocks.shape[2:]
    pt, rhs = u_state.shape
    pd = v_state.shape[1]
    km, kc = mid_left.shape[1], coarse_left.shape[1]
    kt = km + 2 * kc
    row_span, col_span = mid_left.shape[2], mid_right.shape[3]
    row_groups, col_groups = row_span // clp, col_span // clq
    unroll = 16 if slots % 16 == 0 else 1
    in_hbm = pl.BlockSpec(memory_space=pltpu.HBM)
    vmem = pl.BlockSpec(memory_space=pltpu.VMEM)
    dma = pltpu.SemaphoreType.DMA
    row_sem, col_sem = dma((n_row,)), dma((n_col,))
    whole = n_row * n_col <= WHOLE_LIMIT
    last_sem = dma((n_row * n_col,)) if whole else col_sem
    sums = (n_col, n_row, rhs) if whole else (n_row, 8, rhs)
    scratch = [
        pltpu.SMEM(near_rows.shape, jnp.int32),
        pltpu.SMEM(near_cols.shape, jnp.int32),
        pltpu.SMEM(near_count.shape, jnp.int32),
        pltpu.SMEM(mid_rank.shape, jnp.int32),
        pltpu.SMEM(coarse_rank.shape, jnp.int32),
        pltpu.VMEM((slots, 3, clp, clq), bf16),
        pltpu.VMEM((pt, rhs), f32),
        pltpu.VMEM((3, pd, rhs), f32),
        pltpu.VMEM((1, rhs), f32),
        pltpu.VMEM((kt, row_span), bf16),
        pltpu.VMEM((row_span, kt), bf16),
        pltpu.VMEM((3, kt, col_span), bf16),
        pltpu.VMEM((n_row, 3, pd, rhs), bf16),
        pltpu.VMEM((n_row, 3, kc, pd), bf16),
        pltpu.VMEM((row_groups, clp, rhs), f32),
        pltpu.VMEM((n_col, pt, rhs), bf16),
        pltpu.VMEM((n_col, pt, rhs), bf16),
        pltpu.VMEM((n_col, pt, rhs), bf16),
        pltpu.VMEM((row_groups, rhs, clp), bf16),
        pltpu.VMEM((n_row, 8, rhs), f32),
        pltpu.VMEM((col_groups, 3, rhs, clq), f32),
        pltpu.VMEM((n_row, 3, pd, rhs), bf16),
        pltpu.VMEM((n_row, 3, pd, rhs), bf16),
        pltpu.VMEM((n_col, 8, rhs), f32),
        dma((slots,)),
        dma((13,)),
        row_sem,
        row_sem,
        row_sem,
        row_sem,
        col_sem,
        col_sem,
        col_sem,
        col_sem,
        row_sem,
        row_sem,
        row_sem,
        row_sem,
        last_sem,
        last_sem,
        row_sem,
        row_sem,
    ]
    held = pl.pallas_call(
        functools.partial(kernel, (n_row, n_col, unroll)),
        out_shape=(
            pltpu.VMEM((pt, rhs), f32),
            pltpu.VMEM((3, pd, rhs), f32),
            pltpu.VMEM((1, rhs), f32),
            pltpu.VMEM(sums, f32),
        ),
        in_specs=[in_hbm] * 13,
        out_specs=(vmem,) * 4,
        scratch_shapes=scratch,
        compiler_params=pltpu.CompilerParams(
            collective_id=0, has_side_effects=True, vmem_limit_bytes=60 * 1024 * 1024
        ),
        name="lsqr",
    )(
        near_rows,
        near_cols,
        near_count,
        mid_rank,
        coarse_rank,
        u_state,
        v_state,
        alpha_prev.reshape(1, rhs),
        jnp.transpose(near_blocks[0, 0], (0, 2, 1, 3)),
        mid_left[0],
        jnp.transpose(mid_right[0], (1, 0, 2)),
        coarse_left[0],
        jnp.transpose(coarse_right, (1, 0, 2)),
    )
    return pl.pallas_call(
        functools.partial(finish, 3 * pd * n_row * n_col),
        out_shape=(
            jax.ShapeDtypeStruct((pt, rhs), f32),
            jax.ShapeDtypeStruct((3, pd, rhs), f32),
            jax.ShapeDtypeStruct((2, rhs), f32),
        ),
        in_specs=[vmem] * 4,
        out_specs=(vmem,) * 3,
        name="finish",
    )(*[pltpu.with_memory_space_constraint(value, pltpu.VMEM) for value in held])


def solution(mesh):
    placed = (
        P(("row", "col"), None),
        P(None, ("col", "row"), None),
        P(),
        P("row", "col", None, None, None, None),
        P("row", "col", None),
        P("row", "col", None),
        P("row", "col"),
        P("col", None, "row"),
        P("row", None, None, "col"),
        P("row", "col"),
        P("col", None, "row"),
        P(None, None, ("col", "row")),
        P("col"),
    )
    return jax.shard_map(
        functools.partial(per_device, mesh.shape["row"], mesh.shape["col"]),
        mesh=mesh,
        in_specs=placed,
        out_specs=(P(("row", "col"), None), P(None, ("col", "row"), None), P()),
        check_vma=False,
    )
```

```python
import functools

import jax
import jax.numpy as jnp
from jax import lax
from jax.experimental import pallas as pl
from jax.experimental.pallas import tpu as pltpu
from jax.sharding import PartitionSpec as P

tiny_add = 1e-06
MESH = pl.DeviceIdType.MESH
f32, bf16 = jnp.float32, jnp.bfloat16
WHOLE_LIMIT = 64


def fold(values):
    return (values * values).reshape(values.shape[0] // 8, 8, values.shape[1]).sum(axis=0)


def turn(values):
    return jnp.transpose(values.astype(f32), (1, 0))


def kernel(
    sizes,
    rows_hbm,
    cols_hbm,
    count_hbm,
    mid_rank_hbm,
    coarse_rank_hbm,
    u_hbm,
    v_hbm,
    alpha_hbm,
    near_hbm,
    mid_left_hbm,
    mid_right_hbm,
    coarse_left_hbm,
    coarse_right_hbm,
    u_out,
    v_out,
    beta_out,
    vsq_all,
    rows_smem,
    cols_smem,
    count_smem,
    mid_rank_smem,
    coarse_rank_smem,
    near,
    u_old,
    v_old,
    alpha_old,
    left,
    left_turned,
    right,
    slip,
    coarse_all,
    part_codes,
    weights,
    dense,
    dense_turned,
    fsend,
    frecv,
    ug,
    sq,
    bsend,
    brecv,
    vsq_col,
    near_sem,
    in_sem,
    slip_send,
    slip_recv,
    part_send,
    part_recv,
    coarse_send,
    coarse_recv,
    f_send,
    f_recv,
    u_send,
    u_recv,
    sq_send,
    sq_recv,
    b_send,
    b_recv,
    vc_send,
    vc_recv,
    vr_send,
    vr_recv,
):
    n_row, n_col = sizes
    me_r, me_c = lax.axis_index("row"), lax.axis_index("col")
    slots, _, clp, clq = near.shape
    pt, rhs = u_old.shape
    pd = v_old.shape[1]
    km, kc = mid_left_hbm.shape[0], coarse_left_hbm.shape[0]
    kt = km + kc
    row_span, col_span = left.shape[1], right.shape[2]
    row_groups, col_groups = row_span // clp, col_span // clq
    per_col = clq // pd
    spots = row_groups * col_groups
    bunch = 8 if spots % 8 == 0 else spots
    tile = 32

    def row_peer(step):
        return lax.rem(me_r + step, n_row)

    def far_first(me, count, step):
        upper = me >= count // 2
        own = jnp.where(upper, me, count - 1 - me)
        place = step - 1 + (step - 1 >= own).astype(jnp.int32)
        return jnp.where(upper, place, count - 1 - place)

    def col_peer(step):
        return far_first(me_c, n_col, step)

    loads = [
        pltpu.make_async_copy(src, dst, in_sem.at[place])
        for place, (src, dst) in enumerate(
            [
                (v_hbm, v_old),
                (coarse_right_hbm, coarse_all.at[me_r]),
                (rows_hbm, rows_smem),
                (cols_hbm, cols_smem),
                (count_hbm, count_smem),
                (mid_rank_hbm, mid_rank_smem),
                (coarse_rank_hbm, coarse_rank_smem),
                (mid_right_hbm, right.at[:, 0:km, :]),
                (mid_left_hbm, left.at[0:km, :]),
                (coarse_left_hbm, left.at[km:kt, :]),
                (u_hbm, u_old),
                (alpha_hbm, alpha_old),
            ]
        )
    ]
    loads[0].start()
    loads[1].start()

    barrier = pltpu.get_barrier_semaphore()
    for step in range(1, n_col):
        pl.semaphore_signal(barrier, device_id={"col": col_peer(step)}, device_id_type=MESH)
    for step in range(1, n_row):
        pl.semaphore_signal(barrier, device_id={"row": row_peer(step)}, device_id_type=MESH)
    pieces = near_sem.shape[0]
    share = slots // pieces
    near_loads = [
        pltpu.make_async_copy(
            near_hbm.at[pl.ds(piece * share, share)], near.at[pl.ds(piece * share, share)], near_sem.at[piece]
        )
        for piece in range(pieces)
    ]
    for load in near_loads:
        load.start()
    for load in loads[2:]:
        load.start()

    def exchange(axis, me, count, peer, source, target, send_sem, recv_sem, steps=None):
        copies = [
            pltpu.make_async_remote_copy(
                src_ref=source(peer(step)),
                dst_ref=target,
                send_sem=send_sem.at[step - 1],
                recv_sem=recv_sem.at[me],
                device_id={axis: peer(step)},
                device_id_type=MESH,
            )
            for step in range(1, count)
        ]
        for copy in copies:
            copy.start()
        incoming = [
            pltpu.make_async_remote_copy(
                src_ref=source(peer(step)),
                dst_ref=target,
                send_sem=send_sem.at[step - 1],
                recv_sem=recv_sem.at[peer(step)],
                device_id={axis: peer(step)},
                device_id_type=MESH,
            )
            for step in range(1, count)
        ]
        return copies, incoming

    def across_rows(source, target, send_sem, recv_sem):
        return exchange("row", me_r, n_row, row_peer, source, target, send_sem, recv_sem)

    def across_cols(source, target, send_sem, recv_sem):
        return exchange("col", me_c, n_col, col_peer, source, target, send_sem, recv_sem)

    def arrived(copies):
        for copy in copies[1]:
            copy.wait_recv()

    loads[0].wait()
    slip[me_r] = v_old[...].astype(bf16)
    loads[1].wait()
    own_codes = jnp.zeros((kc, rhs), f32)
    for k in range(3):
        own_codes = own_codes + jnp.dot(coarse_all[me_r, k], slip[me_r, k], preferred_element_type=f32)
    part_codes[me_r] = own_codes.astype(bf16)
    pl.semaphore_wait(barrier, n_row + n_col - 2)
    sent_slip = across_rows(lambda peer: slip.at[me_r], slip.at[me_r], slip_send, slip_recv)
    sent_part = across_rows(
        lambda peer: part_codes.at[me_r], part_codes.at[me_r], part_send, part_recv
    )
    for load in loads[2:]:
        load.wait()
    spot_of = lax.broadcasted_iota(jnp.int32, (spots, rhs), 0)
    for slot in range(slots):
        spot = cols_smem[0, 0, slot] * row_groups + rows_smem[0, 0, slot]
        spot = jnp.where(slot < count_smem[0, 0], spot, -1)
        weights[slot] = jnp.where(spot_of == spot, 1.0, 0.0).astype(f32)
    for group in range(row_groups):
        span = slice(group * clp, (group + 1) * clp)
        left_turned[span, :] = turn(left[:, span]).astype(bf16)
    for load in near_loads:
        load.wait()
    chunks = clp // tile

    def build(step, carry):
        chunk, k, first = step % chunks, (step // chunks) % 3, (step // (3 * chunks)) * bunch
        at = pl.multiple_of(chunk * tile, tile)
        sums = [jnp.zeros((tile, clq), f32)] * bunch
        for slot in range(slots):
            block = near[slot, k, pl.ds(at, tile), :].astype(f32)
            for place in range(bunch):
                sums[place] = sums[place] + block * weights[slot, pl.ds(first + place, 1), :]
        for place in range(bunch):
            spot = first + place
            group, wide = spot % row_groups, spot // row_groups
            dense[
                pl.ds(pl.multiple_of(group * clp + at, tile), tile),
                pl.ds(pl.multiple_of((wide * 3 + k) * clq, clq), clq),
            ] = sums[place].astype(bf16)
        return carry

    lax.fori_loop(0, spots // bunch * 3 * chunks, build, 0)
    arrived(sent_slip)
    sent_coarse = across_rows(
        lambda peer: coarse_all.at[me_r], coarse_all.at[me_r], coarse_send, coarse_recv
    )

    codes = jnp.zeros((km, rhs), f32)
    for k in range(3):
        codes = codes + jnp.dot(
            right[k, 0:km, :], slip[:, k].reshape(n_row * pd, rhs), preferred_element_type=f32
        )
    place = lax.broadcasted_iota(jnp.int32, (km, rhs), 0)
    codes = jnp.where(place < mid_rank_smem[0, 0], codes, 0.0).astype(bf16)
    arrived(sent_part)
    coarse_codes = jnp.zeros((kc, rhs), f32)
    for peer in range(n_row):
        coarse_codes = coarse_codes + part_codes[peer].astype(f32)
    place = lax.broadcasted_iota(jnp.int32, (kc, rhs), 0)
    coarse_codes = jnp.where(place < coarse_rank_smem[0], coarse_codes, 0.0).astype(bf16)
    codes = jnp.concatenate([codes, coarse_codes], axis=0)
    gathered = jnp.concatenate(
        [
            slip[wide * per_col : (wide + 1) * per_col, k].reshape(clq, rhs)
            for wide in range(col_groups)
            for k in range(3)
        ],
        axis=0,
    )
    wave = min(row_span, 512)
    for group in range(row_span // wave):
        span = slice(group * wave, (group + 1) * wave)
        value = jnp.dot(dense[span, :], gathered, preferred_element_type=f32)
        value = value + jnp.dot(left_turned[span, :], codes, preferred_element_type=f32)
        fsend[group * wave // pt : (group + 1) * wave // pt] = value.astype(bf16).reshape(
            wave // pt, pt, rhs
        )
    sent_f = across_cols(lambda peer: fsend.at[peer], frecv.at[me_c], f_send, f_recv)
    frecv[me_c] = fsend[me_c]

    arrived(sent_coarse)
    for peer in range(n_row):
        for k in range(3):
            right[k, km:kt, peer * pd : (peer + 1) * pd] = coarse_all[peer, k]
    place = lax.broadcasted_iota(jnp.int32, (kt, row_span), 0)
    limit = jnp.where(place < km, mid_rank_smem[0, 0], coarse_rank_smem[0] + km)
    left[...] = jnp.where(place < limit, left[...].astype(f32), 0.0).astype(bf16)

    def turn_over(step, carry):
        k, wide = step % 3, step // 3
        rank_turned = turn(right[k, :, pl.ds(pl.multiple_of(wide * clq, clq), clq)]).astype(bf16)
        for group in range(row_groups):
            span = slice(group * clp, (group + 1) * clp)
            value = jnp.dot(rank_turned, left[:, span], preferred_element_type=f32)
            value = value + turn(dense[span, pl.ds(pl.multiple_of(step * clq, clq), clq)])
            dense_turned[step, :, span] = value.astype(bf16)
        return carry

    lax.fori_loop(0, 3 * col_groups, turn_over, 0)

    arrived(sent_f)
    u_hat = -alpha_old[...] * u_old[...]
    for peer in range(n_col):
        u_hat = u_hat + frecv[peer].astype(f32)
    ug[me_c] = u_hat.astype(bf16)
    sent_u = across_cols(lambda peer: ug.at[me_c], ug.at[me_c], u_send, u_recv)
    u_old[...] = u_hat
    arrived(sent_u)

    gathered = ug[...].reshape(row_span, rhs)
    own_wide = me_r // per_col
    sent_b, incoming_b = [], []
    for turn_index in range(col_groups):
        wide = lax.rem(own_wide + 1 + turn_index, col_groups)
        for k in range(3):
            value = jnp.dot(dense_turned[wide * 3 + k], gathered, preferred_element_type=f32)
            value = value.astype(bf16).reshape(per_col, pd, rhs)
            for part in range(per_col):
                bsend[wide * per_col + part, k] = value[part]
        last = turn_index == col_groups - 1
        for part in range(per_col):
            if last:
                if part == 0:
                    continue
                peer = wide * per_col + lax.rem(lax.rem(me_r, per_col) + part, per_col)
            else:
                peer = wide * per_col + part
            slot = turn_index * per_col + part
            copy = pltpu.make_async_remote_copy(
                src_ref=bsend.at[peer],
                dst_ref=brecv.at[me_r],
                send_sem=b_send.at[slot],
                recv_sem=b_recv.at[me_r],
                device_id={"row": peer},
                device_id_type=MESH,
            )
            copy.start()
            sent_b.append(copy)
            incoming_b.append(
                pltpu.make_async_remote_copy(
                    src_ref=bsend.at[peer],
                    dst_ref=brecv.at[me_r],
                    send_sem=b_send.at[slot],
                    recv_sem=b_recv.at[peer],
                    device_id={"row": peer},
                    device_id_type=MESH,
                )
            )
        if turn_index == 0:
            sq[me_r] = fold(gathered.astype(f32))
            sent_sq = across_rows(lambda peer: sq.at[me_r], sq.at[me_r], sq_send, sq_recv)
    brecv[me_r] = bsend[me_r]
    sent_b = (sent_b, incoming_b)
    arrived(sent_sq)
    square_sum = jnp.zeros((8, rhs), f32)
    for peer in range(n_row):
        square_sum = square_sum + sq[peer]
    points = pt * n_row * n_col
    beta = jnp.sqrt(jnp.sum(square_sum, axis=0, keepdims=True) / points + tiny_add)
    beta_out[...] = beta
    u_out[...] = u_old[...] / beta
    arrived(sent_b)
    v_squares = jnp.zeros((8, rhs), f32)
    for k in range(3):
        total = jnp.zeros((pd, rhs), f32)
        for peer in range(n_row):
            total = total + brecv[peer, k].astype(f32)
        v_hat = total / beta - beta * v_old[k]
        v_out[k] = v_hat
        v_squares = v_squares + fold(v_hat)
    sent_v = []
    if n_row * n_col <= WHOLE_LIMIT:
        others = [(a, b) for b in range(n_col) for a in range(n_row)][1:]
        far = [(lax.rem(me_r + a, n_row), lax.rem(me_c + b, n_col)) for a, b in others]
        vsq_all[me_c, pl.ds(me_r, 1)] = jnp.sum(v_squares, axis=0, keepdims=True)

        def row_sum(place, row, col):
            return pltpu.make_async_remote_copy(
                src_ref=vsq_all.at[me_c, pl.ds(me_r, 1)],
                dst_ref=vsq_all.at[me_c, pl.ds(me_r, 1)],
                send_sem=vc_send.at[place],
                recv_sem=vc_recv.at[place],
                device_id=(row, col),
                device_id_type=MESH,
            )

        for place in reversed(range(len(far))):
            copy = row_sum(place, *far[place])
            copy.start()
            sent_v.append(copy)
        for copy in sent_v:
            copy.wait_recv()
    else:
        vsq_col[me_c] = v_squares
        sent_vc = across_cols(lambda peer: vsq_col.at[me_c], vsq_col.at[me_c], vc_send, vc_recv)
        arrived(sent_vc)
        v_squares = jnp.zeros((8, rhs), f32)
        for peer in range(n_col):
            v_squares = v_squares + vsq_col[peer]
        vsq_all[me_r] = v_squares
        sent_vr = across_rows(lambda peer: vsq_all.at[me_r], vsq_all.at[me_r], vr_send, vr_recv)
        arrived(sent_vr)
        sent_v = sent_vc[0] + sent_vr[0]
    for copies in (sent_slip, sent_part, sent_coarse, sent_f, sent_u, sent_sq, sent_b):
        for copy in copies[0]:
            copy.wait_send()
    for copy in sent_v:
        copy.wait_send()


def finish(unknowns, u_ref, v_ref, beta_ref, squares_ref, u_out, v_out, norms_out):
    total = jnp.zeros(squares_ref.shape[1:], f32)
    for peer in range(squares_ref.shape[0]):
        total = total + squares_ref[peer]
    alpha = jnp.sqrt(jnp.sum(total, axis=0, keepdims=True) / unknowns + tiny_add)
    norms_out[0:1, :] = beta_ref[...]
    norms_out[1:2, :] = alpha
    u_out[...] = u_ref[...]
    v_out[...] = v_ref[...] / alpha


def per_device(
    n_row,
    n_col,
    u_state,
    v_state,
    alpha_prev,
    near_blocks,
    near_rows,
    near_cols,
    near_count,
    mid_left,
    mid_right,
    mid_rank,
    coarse_left,
    coarse_right,
    coarse_rank,
):
    slots, clp, _, clq = near_blocks.shape[2:]
    pt, rhs = u_state.shape
    pd = v_state.shape[1]
    km, kc = mid_left.shape[1], coarse_left.shape[1]
    kt = km + kc
    row_span, col_span = mid_left.shape[2], mid_right.shape[3]
    row_groups, col_groups = row_span // clp, col_span // clq
    in_hbm = pl.BlockSpec(memory_space=pltpu.HBM)
    vmem = pl.BlockSpec(memory_space=pltpu.VMEM)
    dma = pltpu.SemaphoreType.DMA
    row_sem, col_sem = dma((n_row,)), dma((n_col,))
    whole = n_row * n_col <= WHOLE_LIMIT
    last_sem = dma((n_row * n_col,)) if whole else col_sem
    sums = (n_col, n_row, rhs) if whole else (n_row, 8, rhs)
    scratch = [
        pltpu.SMEM(near_rows.shape, jnp.int32),
        pltpu.SMEM(near_cols.shape, jnp.int32),
        pltpu.SMEM(near_count.shape, jnp.int32),
        pltpu.SMEM(mid_rank.shape, jnp.int32),
        pltpu.SMEM(coarse_rank.shape, jnp.int32),
        pltpu.VMEM((slots, 3, clp, clq), bf16),
        pltpu.VMEM((pt, rhs), f32),
        pltpu.VMEM((3, pd, rhs), f32),
        pltpu.VMEM((1, rhs), f32),
        pltpu.VMEM((kt, row_span), bf16),
        pltpu.VMEM((row_span, kt), bf16),
        pltpu.VMEM((3, kt, col_span), bf16),
        pltpu.VMEM((n_row, 3, pd, rhs), bf16),
        pltpu.VMEM((n_row, 3, kc, pd), bf16),
        pltpu.VMEM((n_row, kc, rhs), bf16),
        pltpu.VMEM((slots, row_groups * col_groups, rhs), f32),
        pltpu.VMEM((row_span, 3 * col_span), bf16),
        pltpu.VMEM((3 * col_groups, clq, row_span), bf16),
        pltpu.VMEM((n_col, pt, rhs), bf16),
        pltpu.VMEM((n_col, pt, rhs), bf16),
        pltpu.VMEM((n_col, pt, rhs), bf16),
        pltpu.VMEM((n_row, 8, rhs), f32),
        pltpu.VMEM((n_row, 3, pd, rhs), bf16),
        pltpu.VMEM((n_row, 3, pd, rhs), bf16),
        pltpu.VMEM((n_col, 8, rhs), f32),
        dma((4 if slots % 4 == 0 else 1,)),
        dma((12,)),
        row_sem,
        row_sem,
        row_sem,
        row_sem,
        row_sem,
        row_sem,
        col_sem,
        col_sem,
        col_sem,
        col_sem,
        row_sem,
        row_sem,
        row_sem,
        row_sem,
        last_sem,
        last_sem,
        row_sem,
        row_sem,
    ]
    held = pl.pallas_call(
        functools.partial(kernel, (n_row, n_col)),
        out_shape=(
            pltpu.VMEM((pt, rhs), f32),
            pltpu.VMEM((3, pd, rhs), f32),
            pltpu.VMEM((1, rhs), f32),
            pltpu.VMEM(sums, f32),
        ),
        in_specs=[in_hbm] * 13,
        out_specs=(vmem,) * 4,
        scratch_shapes=scratch,
        compiler_params=pltpu.CompilerParams(
            collective_id=0, has_side_effects=True, vmem_limit_bytes=60 * 1024 * 1024
        ),
        name="lsqr",
    )(
        near_rows,
        near_cols,
        near_count,
        mid_rank,
        coarse_rank,
        u_state,
        v_state,
        alpha_prev.reshape(1, rhs),
        jnp.transpose(near_blocks[0, 0], (0, 2, 1, 3)),
        mid_left[0],
        jnp.transpose(mid_right[0], (1, 0, 2)),
        coarse_left[0],
        jnp.transpose(coarse_right, (1, 0, 2)),
    )
    return pl.pallas_call(
        functools.partial(finish, 3 * pd * n_row * n_col),
        out_shape=(
            jax.ShapeDtypeStruct((pt, rhs), f32),
            jax.ShapeDtypeStruct((3, pd, rhs), f32),
            jax.ShapeDtypeStruct((2, rhs), f32),
        ),
        in_specs=[vmem] * 4,
        out_specs=(vmem,) * 3,
        name="finish",
    )(*[pltpu.with_memory_space_constraint(value, pltpu.VMEM) for value in held])


def solution(mesh):
    placed = (
        P(("row", "col"), None),
        P(None, ("col", "row"), None),
        P(),
        P("row", "col", None, None, None, None),
        P("row", "col", None),
        P("row", "col", None),
        P("row", "col"),
        P("col", None, "row"),
        P("row", None, None, "col"),
        P("row", "col"),
        P("col", None, "row"),
        P(None, None, ("col", "row")),
        P("col"),
    )
    return jax.shard_map(
        functools.partial(per_device, mesh.shape["row"], mesh.shape["col"]),
        mesh=mesh,
        in_specs=placed,
        out_specs=(P(("row", "col"), None), P(None, ("col", "row"), None), P()),
        check_vma=False,
    )
```

```python
import functools

import jax
import jax.numpy as jnp
from jax import lax
from jax.experimental import pallas as pl
from jax.experimental.pallas import tpu as pltpu
from jax.sharding import PartitionSpec as P

tiny_add = 1e-06
MESH = pl.DeviceIdType.MESH
f32, bf16 = jnp.float32, jnp.bfloat16
WHOLE_LIMIT = 64
COARSE, SLIP, SUMS, LEFT, SQUARES, BACK, ALL, COLS, PARTS = range(9)


def fold(values):
    return (values * values).reshape(values.shape[0] // 8, 8, values.shape[1]).sum(axis=0)


def turn(values):
    return jnp.transpose(values.astype(f32), (1, 0))


def kernel(
    sizes,
    rows_hbm,
    cols_hbm,
    count_hbm,
    mid_rank_hbm,
    coarse_rank_hbm,
    u_hbm,
    v_hbm,
    alpha_hbm,
    near_hbm,
    mid_left_hbm,
    mid_right_hbm,
    coarse_left_hbm,
    coarse_right_hbm,
    u_out,
    v_out,
    beta_out,
    vsq_all,
    rows_smem,
    cols_smem,
    count_smem,
    mid_rank_smem,
    coarse_rank_smem,
    near,
    u_old,
    v_old,
    alpha_old,
    left,
    left_turned,
    right,
    slip,
    coarse_all,
    part_codes,
    weights,
    dense,
    dense_turned,
    fsend,
    frecv,
    ug,
    sq,
    bsend,
    brecv,
    vsq_col,
    near_sem,
    in_sem,
    send_sem,
    recv_sem,
):
    n_row, n_col = sizes
    me_r, me_c = lax.axis_index("row"), lax.axis_index("col")
    slots, _, clp, clq = near.shape
    pt, rhs = u_old.shape
    pd = v_old.shape[1]
    km, kc = mid_left_hbm.shape[0], coarse_left_hbm.shape[0]
    kt = km + kc
    row_span, col_span = left.shape[1], right.shape[2]
    row_groups, col_groups = row_span // clp, col_span // clq
    per_col = clq // pd
    spots = row_groups * col_groups
    bunch = 8 if spots % 8 == 0 else spots
    tile = 32

    def row_peer(step):
        return lax.rem(me_r + step, n_row)

    def far_first(me, count, step):
        upper = me >= count // 2
        own = jnp.where(upper, me, count - 1 - me)
        place = step - 1 + (step - 1 >= own).astype(jnp.int32)
        return jnp.where(upper, place, count - 1 - place)

    def col_peer(step):
        return far_first(me_c, n_col, step)

    loads = [
        pltpu.make_async_copy(src, dst, in_sem.at[place])
        for place, (src, dst) in enumerate(
            [
                (v_hbm, v_old),
                (coarse_right_hbm, coarse_all.at[me_r]),
                (rows_hbm, rows_smem),
                (cols_hbm, cols_smem),
                (count_hbm, count_smem),
                (mid_rank_hbm, mid_rank_smem),
                (coarse_rank_hbm, coarse_rank_smem),
                (mid_right_hbm, right.at[:, 0:km, :]),
                (mid_left_hbm, left.at[0:km, :]),
                (coarse_left_hbm, left.at[km:kt, :]),
                (u_hbm, u_old),
                (alpha_hbm, alpha_old),
            ]
        )
    ]
    loads[0].start()
    loads[1].start()

    barrier = pltpu.get_barrier_semaphore()
    for step in range(1, n_col):
        pl.semaphore_signal(barrier, device_id={"col": col_peer(step)}, device_id_type=MESH)
    for step in range(1, n_row):
        pl.semaphore_signal(barrier, device_id={"row": row_peer(step)}, device_id_type=MESH)
    pieces = 4 if slots % 4 == 0 else 1
    share = slots // pieces
    near_loads = [
        pltpu.make_async_copy(
            near_hbm.at[pl.ds(piece * share, share)], near.at[pl.ds(piece * share, share)], near_sem
        )
        for piece in range(pieces)
    ]
    for load in near_loads:
        load.start()
    for load in loads[2:]:
        load.start()

    def post(place, device, source, target):
        copy = pltpu.make_async_remote_copy(
            src_ref=source,
            dst_ref=target,
            send_sem=send_sem.at[place],
            recv_sem=recv_sem.at[place],
            device_id=device,
            device_id_type=MESH,
        )
        return copy

    def across_rows(place, source, target):
        for step in range(1, n_row):
            post(place, {"row": row_peer(step)}, source(row_peer(step)), target).start()

    def across_cols(place, source, target):
        for step in range(1, n_col):
            post(place, {"col": col_peer(step)}, source(col_peer(step)), target).start()

    def every(place, buffer, count):
        return post(place, {"row": row_peer(1)}, buffer.at[pl.ds(0, count - 1)], buffer.at[pl.ds(0, count - 1)])

    loads[0].wait()
    slip[me_r] = v_old[...].astype(bf16)
    loads[1].wait()
    own_codes = jnp.zeros((kc, rhs), f32)
    for k in range(3):
        own_codes = own_codes + jnp.dot(coarse_all[me_r, k], slip[me_r, k], preferred_element_type=f32)
    part_codes[me_r] = own_codes.astype(bf16)
    pl.semaphore_wait(barrier, n_row + n_col - 2)
    across_rows(PARTS, lambda peer: part_codes.at[me_r], part_codes.at[me_r])
    across_rows(SLIP, lambda peer: slip.at[me_r], slip.at[me_r])
    for load in loads[2:]:
        load.wait()
    spot_of = lax.broadcasted_iota(jnp.int32, (spots, rhs), 0)
    for slot in range(slots):
        spot = cols_smem[0, 0, slot] * row_groups + rows_smem[0, 0, slot]
        spot = jnp.where(slot < count_smem[0, 0], spot, -1)
        weights[slot] = jnp.where(spot_of == spot, 1.0, 0.0).astype(f32)
    for group in range(row_groups):
        span = slice(group * clp, (group + 1) * clp)
        left_turned[span, :] = turn(left[:, span]).astype(bf16)
    pltpu.make_async_copy(near_hbm, near, near_sem).wait()
    chunks = clp // tile

    def build(step, carry):
        chunk, k, first = step % chunks, (step // chunks) % 3, (step // (3 * chunks)) * bunch
        at = pl.multiple_of(chunk * tile, tile)
        sums = [jnp.zeros((tile, clq), f32)] * bunch
        for slot in range(slots):
            block = near[slot, k, pl.ds(at, tile), :].astype(f32)
            for place in range(bunch):
                sums[place] = sums[place] + block * weights[slot, pl.ds(first + place, 1), :]
        for place in range(bunch):
            spot = first + place
            group, wide = spot % row_groups, spot // row_groups
            dense[
                pl.ds(pl.multiple_of(group * clp + at, tile), tile),
                pl.ds(pl.multiple_of((wide * 3 + k) * clq, clq), clq),
            ] = sums[place].astype(bf16)
        return carry

    lax.fori_loop(0, spots // bunch * 3 * chunks, build, 0)
    across_rows(COARSE, lambda peer: coarse_all.at[me_r], coarse_all.at[me_r])
    every(PARTS, part_codes, n_row).wait_recv()
    coarse_codes = jnp.zeros((kc, rhs), f32)
    for peer in range(n_row):
        coarse_codes = coarse_codes + part_codes[peer].astype(f32)
    place = lax.broadcasted_iota(jnp.int32, (kc, rhs), 0)
    coarse_codes = jnp.where(place < coarse_rank_smem[0], coarse_codes, 0.0).astype(bf16)
    every(SLIP, slip, n_row).wait_recv()
    codes = jnp.zeros((km, rhs), f32)
    for k in range(3):
        codes = codes + jnp.dot(
            right[k, 0:km, :], slip[:, k].reshape(n_row * pd, rhs), preferred_element_type=f32
        )
    place = lax.broadcasted_iota(jnp.int32, (km, rhs), 0)
    codes = jnp.where(place < mid_rank_smem[0, 0], codes, 0.0).astype(bf16)
    codes = jnp.concatenate([codes, coarse_codes], axis=0)
    gathered = jnp.concatenate(
        [
            slip[wide * per_col : (wide + 1) * per_col, k].reshape(clq, rhs)
            for wide in range(col_groups)
            for k in range(3)
        ],
        axis=0,
    )
    wave = min(row_span, 512)
    for group in range(row_span // wave):
        span = slice(group * wave, (group + 1) * wave)
        value = jnp.dot(dense[span, :], gathered, preferred_element_type=f32)
        value = value + jnp.dot(left_turned[span, :], codes, preferred_element_type=f32)
        fsend[group * wave // pt : (group + 1) * wave // pt] = value.astype(bf16).reshape(
            wave // pt, pt, rhs
        )
    across_cols(SUMS, lambda peer: fsend.at[peer], frecv.at[me_c])
    frecv[me_c] = fsend[me_c]

    every(COARSE, coarse_all, n_row).wait_recv()
    for peer in range(n_row):
        for k in range(3):
            right[k, km:kt, peer * pd : (peer + 1) * pd] = coarse_all[peer, k]
    place = lax.broadcasted_iota(jnp.int32, (kt, row_span), 0)
    limit = jnp.where(place < km, mid_rank_smem[0, 0], coarse_rank_smem[0] + km)
    left[...] = jnp.where(place < limit, left[...].astype(f32), 0.0).astype(bf16)

    def turn_over(step, carry):
        k, wide = step % 3, step // 3
        rank_turned = turn(right[k, :, pl.ds(pl.multiple_of(wide * clq, clq), clq)]).astype(bf16)
        for group in range(row_groups):
            span = slice(group * clp, (group + 1) * clp)
            value = jnp.dot(rank_turned, left[:, span], preferred_element_type=f32)
            value = value + turn(dense[span, pl.ds(pl.multiple_of(step * clq, clq), clq)])
            dense_turned[step, :, span] = value.astype(bf16)
        return carry

    lax.fori_loop(0, 3 * col_groups, turn_over, 0)

    every(SUMS, frecv, n_col).wait_recv()
    u_hat = -alpha_old[...] * u_old[...]
    for peer in range(n_col):
        u_hat = u_hat + frecv[peer].astype(f32)
    ug[me_c] = u_hat.astype(bf16)
    across_cols(LEFT, lambda peer: ug.at[me_c], ug.at[me_c])
    u_old[...] = u_hat
    every(LEFT, ug, n_col).wait_recv()

    gathered = ug[...].reshape(row_span, rhs)
    own_wide = me_r // per_col
    for turn_index in range(col_groups):
        wide = lax.rem(own_wide + 1 + turn_index, col_groups)
        for k in range(3):
            value = jnp.dot(dense_turned[wide * 3 + k], gathered, preferred_element_type=f32)
            value = value.astype(bf16).reshape(per_col, pd, rhs)
            for part in range(per_col):
                bsend[wide * per_col + part, k] = value[part]
        last = turn_index == col_groups - 1
        for part in range(per_col):
            if last:
                if part == 0:
                    continue
                peer = wide * per_col + lax.rem(lax.rem(me_r, per_col) + part, per_col)
            else:
                peer = wide * per_col + part
            post(BACK, {"row": peer}, bsend.at[peer], brecv.at[me_r]).start()
        if turn_index == 0:
            sq[me_r] = fold(gathered.astype(f32))
            across_rows(SQUARES, lambda peer: sq.at[me_r], sq.at[me_r])
    brecv[me_r] = bsend[me_r]
    every(SQUARES, sq, n_row).wait_recv()
    square_sum = jnp.zeros((8, rhs), f32)
    for peer in range(n_row):
        square_sum = square_sum + sq[peer]
    points = pt * n_row * n_col
    beta = jnp.sqrt(jnp.sum(square_sum, axis=0, keepdims=True) / points + tiny_add)
    beta_out[...] = beta
    u_out[...] = u_old[...] / beta
    every(BACK, brecv, n_row).wait_recv()
    v_squares = jnp.zeros((8, rhs), f32)
    for k in range(3):
        total = jnp.zeros((pd, rhs), f32)
        for peer in range(n_row):
            total = total + brecv[peer, k].astype(f32)
        v_hat = total / beta - beta * v_old[k]
        v_out[k] = v_hat
        v_squares = v_squares + fold(v_hat)
    if n_row * n_col <= WHOLE_LIMIT:
        others = [(a, b) for b in reversed(range(n_col)) for a in reversed(range(n_row))][:-1]
        own = vsq_all.at[me_c * n_row + me_r]
        vsq_all[me_c * n_row + me_r] = jnp.sum(v_squares, axis=0, keepdims=True)
        for a, b in others:
            post(ALL, (lax.rem(me_r + a, n_row), lax.rem(me_c + b, n_col)), own, own).start()
        every(ALL, vsq_all, n_row * n_col).wait_recv()
    else:
        vsq_col[me_c] = v_squares
        across_cols(COLS, lambda peer: vsq_col.at[me_c], vsq_col.at[me_c])
        every(COLS, vsq_col, n_col).wait_recv()
        v_squares = jnp.zeros((8, rhs), f32)
        for peer in range(n_col):
            v_squares = v_squares + vsq_col[peer]
        vsq_all[me_r] = v_squares
        across_rows(ALL, lambda peer: vsq_all.at[me_r], vsq_all.at[me_r])
        every(ALL, vsq_all, n_row).wait_recv()
        every(COLS, vsq_col, n_col).wait_send()
    for place, buffer in (
        (PARTS, part_codes),
        (COARSE, coarse_all),
        (SLIP, slip),
        (SUMS, fsend),
        (LEFT, ug),
        (SQUARES, sq),
        (BACK, bsend),
        (ALL, vsq_all),
    ):
        every(place, buffer, buffer.shape[0]).wait_send()


def finish(unknowns, u_ref, v_ref, beta_ref, squares_ref, u_out, v_out, norms_out):
    total = jnp.zeros(squares_ref.shape[1:], f32)
    for peer in range(squares_ref.shape[0]):
        total = total + squares_ref[peer]
    alpha = jnp.sqrt(jnp.sum(total, axis=0, keepdims=True) / unknowns + tiny_add)
    norms_out[0:1, :] = beta_ref[...]
    norms_out[1:2, :] = alpha
    u_out[...] = u_ref[...]
    v_out[...] = v_ref[...] / alpha


def per_device(
    n_row,
    n_col,
    u_state,
    v_state,
    alpha_prev,
    near_blocks,
    near_rows,
    near_cols,
    near_count,
    mid_left,
    mid_right,
    mid_rank,
    coarse_left,
    coarse_right,
    coarse_rank,
):
    slots, clp, _, clq = near_blocks.shape[2:]
    pt, rhs = u_state.shape
    pd = v_state.shape[1]
    km, kc = mid_left.shape[1], coarse_left.shape[1]
    kt = km + kc
    row_span, col_span = mid_left.shape[2], mid_right.shape[3]
    row_groups, col_groups = row_span // clp, col_span // clq
    in_hbm = pl.BlockSpec(memory_space=pltpu.HBM)
    vmem = pl.BlockSpec(memory_space=pltpu.VMEM)
    dma = pltpu.SemaphoreType.DMA
    whole = n_row * n_col <= WHOLE_LIMIT
    sums = (n_row * n_col, 1, rhs) if whole else (n_row, 8, rhs)
    scratch = [
        pltpu.SMEM(near_rows.shape, jnp.int32),
        pltpu.SMEM(near_cols.shape, jnp.int32),
        pltpu.SMEM(near_count.shape, jnp.int32),
        pltpu.SMEM(mid_rank.shape, jnp.int32),
        pltpu.SMEM(coarse_rank.shape, jnp.int32),
        pltpu.VMEM((slots, 3, clp, clq), bf16),
        pltpu.VMEM((pt, rhs), f32),
        pltpu.VMEM((3, pd, rhs), f32),
        pltpu.VMEM((1, rhs), f32),
        pltpu.VMEM((kt, row_span), bf16),
        pltpu.VMEM((row_span, kt), bf16),
        pltpu.VMEM((3, kt, col_span), bf16),
        pltpu.VMEM((n_row, 3, pd, rhs), bf16),
        pltpu.VMEM((n_row, 3, kc, pd), bf16),
        pltpu.VMEM((n_row, kc, rhs), bf16),
        pltpu.VMEM((slots, row_groups * col_groups, rhs), f32),
        pltpu.VMEM((row_span, 3 * col_span), bf16),
        pltpu.VMEM((3 * col_groups, clq, row_span), bf16),
        pltpu.VMEM((n_col, pt, rhs), bf16),
        pltpu.VMEM((n_col, pt, rhs), bf16),
        pltpu.VMEM((n_col, pt, rhs), bf16),
        pltpu.VMEM((n_row, 8, rhs), f32),
        pltpu.VMEM((n_row, 3, pd, rhs), bf16),
        pltpu.VMEM((n_row, 3, pd, rhs), bf16),
        pltpu.VMEM((n_col, 8, rhs), f32),
        dma,
        dma((12,)),
        dma((9,)),
        dma((9,)),
    ]
    held = pl.pallas_call(
        functools.partial(kernel, (n_row, n_col)),
        out_shape=(
            pltpu.VMEM((pt, rhs), f32),
            pltpu.VMEM((3, pd, rhs), f32),
            pltpu.VMEM((1, rhs), f32),
            pltpu.VMEM(sums, f32),
        ),
        in_specs=[in_hbm] * 13,
        out_specs=(vmem,) * 4,
        scratch_shapes=scratch,
        compiler_params=pltpu.CompilerParams(
            collective_id=0, has_side_effects=True, vmem_limit_bytes=60 * 1024 * 1024
        ),
        name="lsqr",
    )(
        near_rows,
        near_cols,
        near_count,
        mid_rank,
        coarse_rank,
        u_state,
        v_state,
        alpha_prev.reshape(1, rhs),
        jnp.transpose(near_blocks[0, 0], (0, 2, 1, 3)),
        mid_left[0],
        jnp.transpose(mid_right[0], (1, 0, 2)),
        coarse_left[0],
        jnp.transpose(coarse_right, (1, 0, 2)),
    )
    return pl.pallas_call(
        functools.partial(finish, 3 * pd * n_row * n_col),
        out_shape=(
            jax.ShapeDtypeStruct((pt, rhs), f32),
            jax.ShapeDtypeStruct((3, pd, rhs), f32),
            jax.ShapeDtypeStruct((2, rhs), f32),
        ),
        in_specs=[vmem] * 4,
        out_specs=(vmem,) * 3,
        name="finish",
    )(*[pltpu.with_memory_space_constraint(value, pltpu.VMEM) for value in held])


def solution(mesh):
    placed = (
        P(("row", "col"), None),
        P(None, ("col", "row"), None),
        P(),
        P("row", "col", None, None, None, None),
        P("row", "col", None),
        P("row", "col", None),
        P("row", "col"),
        P("col", None, "row"),
        P("row", None, None, "col"),
        P("row", "col"),
        P("col", None, "row"),
        P(None, None, ("col", "row")),
        P("col"),
    )
    return jax.shard_map(
        functools.partial(per_device, mesh.shape["row"], mesh.shape["col"]),
        mesh=mesh,
        in_specs=placed,
        out_specs=(P(("row", "col"), None), P(None, ("col", "row"), None), P()),
        check_vma=False,
    )
```

```python
import functools

import jax
import jax.numpy as jnp
from jax import lax
from jax.experimental import pallas as pl
from jax.experimental.pallas import tpu as pltpu
from jax.sharding import PartitionSpec as P

tiny_add = 1e-06
MESH = pl.DeviceIdType.MESH
f32, bf16 = jnp.float32, jnp.bfloat16
WHOLE_LIMIT = 64
COARSE, SLIP, SUMS, LEFT, SQUARES, BACK, ALL, COLS, PARTS = range(9)


def fold(values):
    return (values * values).reshape(values.shape[0] // 8, 8, values.shape[1]).sum(axis=0)


def turn(values):
    return jnp.transpose(values.astype(f32), (1, 0))


def kernel(
    sizes,
    rows_hbm,
    cols_hbm,
    count_hbm,
    mid_rank_hbm,
    coarse_rank_hbm,
    u_hbm,
    v_hbm,
    alpha_hbm,
    near_hbm,
    mid_left_hbm,
    mid_right_hbm,
    coarse_left_hbm,
    coarse_right_hbm,
    u_out,
    v_out,
    beta_out,
    vsq_all,
    rows_smem,
    cols_smem,
    count_smem,
    mid_rank_smem,
    coarse_rank_smem,
    near,
    u_old,
    v_old,
    alpha_old,
    left,
    left_turned,
    right,
    slip,
    coarse_all,
    coarse_wide,
    begun,
    part_codes,
    weights,
    dense,
    dense_turned,
    fsend,
    frecv,
    ug,
    sq,
    bsend,
    brecv,
    vsq_col,
    near_sem,
    in_sem,
    send_sem,
    recv_sem,
):
    n_row, n_col = sizes
    me_r, me_c = lax.axis_index("row"), lax.axis_index("col")
    slots, _, clp, clq = near.shape
    pt, rhs = u_old.shape
    pd = v_old.shape[1]
    km, kc = mid_left_hbm.shape[0], coarse_left_hbm.shape[0]
    kt = km + kc
    row_span, col_span = left.shape[1], right.shape[2]
    row_groups, col_groups = row_span // clp, col_span // clq
    per_col = clq // pd
    spots = row_groups * col_groups
    bunch = 8 if spots % 8 == 0 else spots
    tile = 32

    def flipped(me, mask):
        place, bit = me, 1
        while bit <= mask:
            if mask & bit:
                place = place + (1 - 2 * ((me // bit) % 2)) * bit
            bit *= 2
        return place

    if n_col & (n_col - 1):
        col_peers = [lax.rem(me_c + step, n_col) for step in range(1, n_col)]
    else:
        masks = list(range(n_col - 1, 0, -2)) + list(range(n_col - 2, 0, -2))
        col_peers = [flipped(me_c, mask) for mask in masks]
    if n_row % 2:
        row_peers = [lax.rem(me_r + step, n_row) for step in range(1, n_row)]
    else:
        own_chip, core = me_r // 2, lax.rem(me_r, 2)
        row_peers = []
        for step in range(1, n_row // 2):
            chip = lax.rem(own_chip + step, n_row // 2)
            row_peers += [chip * 2 + 1 - core, chip * 2 + core]
        row_peers += [own_chip * 2 + 1 - core]

    loads = [
        pltpu.make_async_copy(src, dst, in_sem.at[place])
        for place, (src, dst) in enumerate(
            [
                (v_hbm, v_old),
                (coarse_right_hbm, coarse_all.at[me_r]),
                (rows_hbm, rows_smem),
                (cols_hbm, cols_smem),
                (count_hbm, count_smem),
                (mid_rank_hbm, mid_rank_smem),
                (coarse_rank_hbm, coarse_rank_smem),
                (mid_right_hbm, right),
                (mid_left_hbm, left.at[0:km, :]),
                (coarse_left_hbm, left.at[km:kt, :]),
                (u_hbm, u_old),
                (alpha_hbm, alpha_old),
            ]
        )
    ]
    loads[0].start()
    loads[1].start()

    barrier = pltpu.get_barrier_semaphore()
    for peer in col_peers:
        pl.semaphore_signal(barrier, device_id={"col": peer}, device_id_type=MESH)
    for peer in row_peers:
        pl.semaphore_signal(barrier, device_id={"row": peer}, device_id_type=MESH)
    pieces = 4 if slots % 4 == 0 else 1
    share = slots // pieces
    near_loads = [
        pltpu.make_async_copy(
            near_hbm.at[pl.ds(piece * share, share)], near.at[pl.ds(piece * share, share)], near_sem
        )
        for piece in range(pieces)
    ]
    for load in near_loads:
        load.start()
    for load in loads[2:]:
        load.start()

    def post(place, device, source, target):
        copy = pltpu.make_async_remote_copy(
            src_ref=source,
            dst_ref=target,
            send_sem=send_sem.at[place],
            recv_sem=recv_sem.at[place],
            device_id=device,
            device_id_type=MESH,
        )
        return copy

    def across_rows(place, source, target):
        for peer in row_peers:
            post(place, {"row": peer}, source(peer), target).start()

    def across_cols(place, source, target):
        for peer in col_peers:
            post(place, {"col": peer}, source(peer), target).start()

    def every(place, buffer, count):
        return post(place, {"row": row_peers[0]}, buffer.at[pl.ds(0, count - 1)], buffer.at[pl.ds(0, count - 1)])

    loads[0].wait()
    slip[me_r] = v_old[...].astype(bf16)
    loads[1].wait()
    own_codes = jnp.zeros((kc, rhs), f32)
    for k in range(3):
        own_codes = own_codes + jnp.dot(coarse_all[me_r, k], slip[me_r, k], preferred_element_type=f32)
    part_codes[me_r] = own_codes.astype(bf16)
    pl.semaphore_wait(barrier, n_row + n_col - 2)
    across_rows(PARTS, lambda peer: part_codes.at[me_r], part_codes.at[me_r])
    across_rows(SLIP, lambda peer: slip.at[me_r], slip.at[me_r])
    for load in loads[2:]:
        load.wait()
    place = lax.broadcasted_iota(jnp.int32, (kt, row_span), 0)
    limit = jnp.where(place < km, mid_rank_smem[0, 0], coarse_rank_smem[0] + km)
    left[...] = jnp.where(place < limit, left[...].astype(f32), 0.0).astype(bf16)
    spot_of = lax.broadcasted_iota(jnp.int32, (spots, rhs), 0)
    for slot in range(slots):
        spot = cols_smem[0, 0, slot] * row_groups + rows_smem[0, 0, slot]
        spot = jnp.where(slot < count_smem[0, 0], spot, -1)
        weights[slot] = jnp.where(spot_of == spot, 1.0, 0.0).astype(f32)
    for group in range(row_groups):
        span = slice(group * clp, (group + 1) * clp)
        left_turned[span, :] = turn(left[:, span]).astype(bf16)
    pltpu.make_async_copy(near_hbm, near, near_sem).wait()
    chunks = clp // tile

    sets = max(1, bunch // row_groups)
    each = bunch // sets

    def build(step, carry):
        chunk, k = step % chunks, (step // chunks) % 3
        first = step // (3 * chunks) * bunch if spots > bunch else 0
        at = pl.multiple_of(chunk * tile, tile)
        sums = [jnp.zeros((tile, clq), f32)] * bunch
        for slot in range(slots):
            block = near[slot, k, pl.ds(at, tile), :].astype(f32)
            for place in range(bunch):
                sums[place] = sums[place] + block * weights[slot, pl.ds(first + place, 1), :]
        for part in range(sets):
            places = range(part * each, (part + 1) * each)
            wide = (first + part * each) // row_groups
            groups = [(first + place) % row_groups for place in places]
            ranks = jnp.concatenate(
                [left_turned[pl.ds(pl.multiple_of(group * clp + at, tile), tile), 0:km] for group in groups], axis=0
            )
            low = jnp.dot(
                ranks, right[k, :, pl.ds(pl.multiple_of(wide * clq, clq), clq)], preferred_element_type=f32
            )
            for number, (place, group) in enumerate(zip(places, groups)):
                dense[
                    pl.ds(pl.multiple_of(group * clp + at, tile), tile),
                    pl.ds(pl.multiple_of((wide * 3 + k) * clq, clq), clq),
                ] = (sums[place] + low[number * tile : (number + 1) * tile]).astype(bf16)
        return carry

    lax.fori_loop(0, spots // bunch * 3 * chunks, build, 0)
    across_rows(COARSE, lambda peer: coarse_all.at[me_r], coarse_all.at[me_r])
    every(PARTS, part_codes, n_row).wait_recv()
    coarse_codes = jnp.zeros((kc, rhs), f32)
    for peer in range(n_row):
        coarse_codes = coarse_codes + part_codes[peer].astype(f32)
    coarse_codes = coarse_codes.astype(bf16)
    wave = min(row_span, 512)
    for group in range(row_span // wave):
        span = slice(group * wave, (group + 1) * wave)
        begun[span, :] = jnp.dot(left_turned[span, km:kt], coarse_codes, preferred_element_type=f32)
    every(SLIP, slip, n_row).wait_recv()
    gathered = jnp.concatenate(
        [
            slip[wide * per_col : (wide + 1) * per_col, k].reshape(clq, rhs)
            for wide in range(col_groups)
            for k in range(3)
        ],
        axis=0,
    )
    for group in range(row_span // wave):
        span = slice(group * wave, (group + 1) * wave)
        value = begun[span, :] + jnp.dot(dense[span, :], gathered, preferred_element_type=f32)
        fsend[group * wave // pt : (group + 1) * wave // pt] = value.astype(bf16).reshape(
            wave // pt, pt, rhs
        )
    across_cols(SUMS, lambda peer: fsend.at[peer], frecv.at[me_c])
    frecv[me_c] = fsend[me_c]

    every(COARSE, coarse_all, n_row).wait_recv()
    for peer in range(n_row):
        for k in range(3):
            coarse_wide[k, :, peer * pd : (peer + 1) * pd] = coarse_all[peer, k]

    def turn_over(step, carry):
        k, wide = step % 3, step // 3
        rank_turned = turn(coarse_wide[k, :, pl.ds(pl.multiple_of(wide * clq, clq), clq)]).astype(bf16)
        for group in range(row_groups):
            span = slice(group * clp, (group + 1) * clp)
            value = jnp.dot(rank_turned, left[km:kt, span], preferred_element_type=f32)
            value = value + turn(dense[span, pl.ds(pl.multiple_of(step * clq, clq), clq)])
            dense_turned[step, :, span] = value.astype(bf16)
        return carry

    lax.fori_loop(0, 3 * col_groups, turn_over, 0)

    every(SUMS, frecv, n_col).wait_recv()
    u_hat = -alpha_old[...] * u_old[...]
    for peer in range(n_col):
        u_hat = u_hat + frecv[peer].astype(f32)
    ug[me_c] = u_hat.astype(bf16)
    across_cols(LEFT, lambda peer: ug.at[me_c], ug.at[me_c])
    u_old[...] = u_hat
    every(LEFT, ug, n_col).wait_recv()

    gathered = ug[...].reshape(row_span, rhs)
    own_wide = me_r // per_col
    for turn_index in range(col_groups):
        wide = lax.rem(own_wide + 1 + turn_index, col_groups)
        for k in range(3):
            value = jnp.dot(dense_turned[wide * 3 + k], gathered, preferred_element_type=f32)
            value = value.astype(bf16).reshape(per_col, pd, rhs)
            for part in range(per_col):
                bsend[wide * per_col + part, k] = value[part]
        last = turn_index == col_groups - 1
        for part in range(1 if last else 0, per_col):
            beside = lax.rem(lax.rem(me_r, per_col) + (part if last else part + 1), per_col)
            peer = wide * per_col + beside
            post(BACK, {"row": peer}, bsend.at[peer], brecv.at[me_r]).start()
        if turn_index == 0:
            sq[me_r] = fold(gathered.astype(f32))
            across_rows(SQUARES, lambda peer: sq.at[me_r], sq.at[me_r])
    brecv[me_r] = bsend[me_r]
    every(SQUARES, sq, n_row).wait_recv()
    square_sum = jnp.zeros((8, rhs), f32)
    for peer in range(n_row):
        square_sum = square_sum + sq[peer]
    points = pt * n_row * n_col
    beta = jnp.sqrt(jnp.sum(square_sum, axis=0, keepdims=True) / points + tiny_add)
    beta_out[...] = beta
    inverse = 1.0 / beta
    u_out[...] = u_old[...] * inverse
    every(BACK, brecv, n_row).wait_recv()
    v_squares = jnp.zeros((8, rhs), f32)
    for k in range(3):
        total = jnp.zeros((pd, rhs), f32)
        for peer in range(n_row):
            total = total + brecv[peer, k].astype(f32)
        v_hat = total * inverse - beta * v_old[k]
        v_out[k] = v_hat
        v_squares = v_squares + fold(v_hat)
    if n_row * n_col <= WHOLE_LIMIT:
        others = [(a, b) for b in reversed(range(n_col)) for a in reversed(range(n_row))][:-1]
        own = vsq_all.at[me_c * n_row + me_r]
        vsq_all[me_c * n_row + me_r] = jnp.sum(v_squares, axis=0, keepdims=True)
        for a, b in others:
            post(ALL, (lax.rem(me_r + a, n_row), lax.rem(me_c + b, n_col)), own, own).start()
        every(ALL, vsq_all, n_row * n_col).wait_recv()
    else:
        vsq_col[me_c] = v_squares
        across_cols(COLS, lambda peer: vsq_col.at[me_c], vsq_col.at[me_c])
        every(COLS, vsq_col, n_col).wait_recv()
        v_squares = jnp.zeros((8, rhs), f32)
        for peer in range(n_col):
            v_squares = v_squares + vsq_col[peer]
        vsq_all[me_r] = v_squares
        across_rows(ALL, lambda peer: vsq_all.at[me_r], vsq_all.at[me_r])
        every(ALL, vsq_all, n_row).wait_recv()
        every(COLS, vsq_col, n_col).wait_send()
    for place, buffer in (
        (PARTS, part_codes),
        (COARSE, coarse_all),
        (SLIP, slip),
        (SUMS, fsend),
        (LEFT, ug),
        (SQUARES, sq),
        (BACK, bsend),
        (ALL, vsq_all),
    ):
        every(place, buffer, buffer.shape[0]).wait_send()


def finish(unknowns, u_ref, v_ref, beta_ref, squares_ref, u_out, v_out, norms_out):
    total = jnp.zeros(squares_ref.shape[1:], f32)
    for peer in range(squares_ref.shape[0]):
        total = total + squares_ref[peer]
    alpha = jnp.sqrt(jnp.sum(total, axis=0, keepdims=True) / unknowns + tiny_add)
    norms_out[0:1, :] = beta_ref[...]
    norms_out[1:2, :] = alpha
    u_out[...] = u_ref[...]
    v_out[...] = v_ref[...] / alpha


def per_device(
    n_row,
    n_col,
    u_state,
    v_state,
    alpha_prev,
    near_blocks,
    near_rows,
    near_cols,
    near_count,
    mid_left,
    mid_right,
    mid_rank,
    coarse_left,
    coarse_right,
    coarse_rank,
):
    slots, clp, _, clq = near_blocks.shape[2:]
    pt, rhs = u_state.shape
    pd = v_state.shape[1]
    km, kc = mid_left.shape[1], coarse_left.shape[1]
    kt = km + kc
    row_span, col_span = mid_left.shape[2], mid_right.shape[3]
    row_groups, col_groups = row_span // clp, col_span // clq
    in_hbm = pl.BlockSpec(memory_space=pltpu.HBM)
    vmem = pl.BlockSpec(memory_space=pltpu.VMEM)
    dma = pltpu.SemaphoreType.DMA
    whole = n_row * n_col <= WHOLE_LIMIT
    sums = (n_row * n_col, 1, rhs) if whole else (n_row, 8, rhs)
    scratch = [
        pltpu.SMEM(near_rows.shape, jnp.int32),
        pltpu.SMEM(near_cols.shape, jnp.int32),
        pltpu.SMEM(near_count.shape, jnp.int32),
        pltpu.SMEM(mid_rank.shape, jnp.int32),
        pltpu.SMEM(coarse_rank.shape, jnp.int32),
        pltpu.VMEM((slots, 3, clp, clq), bf16),
        pltpu.VMEM((pt, rhs), f32),
        pltpu.VMEM((3, pd, rhs), f32),
        pltpu.VMEM((1, rhs), f32),
        pltpu.VMEM((kt, row_span), bf16),
        pltpu.VMEM((row_span, kt), bf16),
        pltpu.VMEM((3, km, col_span), bf16),
        pltpu.VMEM((n_row, 3, pd, rhs), bf16),
        pltpu.VMEM((n_row, 3, kc, pd), bf16),
        pltpu.VMEM((3, kc, col_span), bf16),
        pltpu.VMEM((row_span, rhs), f32),
        pltpu.VMEM((n_row, kc, rhs), bf16),
        pltpu.VMEM((slots, row_groups * col_groups, rhs), f32),
        pltpu.VMEM((row_span, 3 * col_span), bf16),
        pltpu.VMEM((3 * col_groups, clq, row_span), bf16),
        pltpu.VMEM((n_col, pt, rhs), bf16),
        pltpu.VMEM((n_col, pt, rhs), bf16),
        pltpu.VMEM((n_col, pt, rhs), bf16),
        pltpu.VMEM((n_row, 8, rhs), f32),
        pltpu.VMEM((n_row, 3, pd, rhs), bf16),
        pltpu.VMEM((n_row, 3, pd, rhs), bf16),
        pltpu.VMEM((n_col, 8, rhs), f32),
        dma,
        dma((12,)),
        dma((9,)),
        dma((9,)),
    ]
    held = pl.pallas_call(
        functools.partial(kernel, (n_row, n_col)),
        out_shape=(
            pltpu.VMEM((pt, rhs), f32),
            pltpu.VMEM((3, pd, rhs), f32),
            pltpu.VMEM((1, rhs), f32),
            pltpu.VMEM(sums, f32),
        ),
        in_specs=[in_hbm] * 13,
        out_specs=(vmem,) * 4,
        scratch_shapes=scratch,
        compiler_params=pltpu.CompilerParams(
            collective_id=0, has_side_effects=True, vmem_limit_bytes=60 * 1024 * 1024
        ),
        name="lsqr",
    )(
        near_rows,
        near_cols,
        near_count,
        mid_rank,
        coarse_rank,
        u_state,
        v_state,
        alpha_prev.reshape(1, rhs),
        jnp.transpose(near_blocks[0, 0], (0, 2, 1, 3)),
        mid_left[0],
        jnp.transpose(mid_right[0], (1, 0, 2)),
        coarse_left[0],
        jnp.transpose(coarse_right, (1, 0, 2)),
    )
    return pl.pallas_call(
        functools.partial(finish, 3 * pd * n_row * n_col),
        out_shape=(
            jax.ShapeDtypeStruct((pt, rhs), f32),
            jax.ShapeDtypeStruct((3, pd, rhs), f32),
            jax.ShapeDtypeStruct((2, rhs), f32),
        ),
        in_specs=[vmem] * 4,
        out_specs=(vmem,) * 3,
        name="finish",
    )(*[pltpu.with_memory_space_constraint(value, pltpu.VMEM) for value in held])


def solution(mesh):
    placed = (
        P(("row", "col"), None),
        P(None, ("col", "row"), None),
        P(),
        P("row", "col", None, None, None, None),
        P("row", "col", None),
        P("row", "col", None),
        P("row", "col"),
        P("col", None, "row"),
        P("row", None, None, "col"),
        P("row", "col"),
        P("col", None, "row"),
        P(None, None, ("col", "row")),
        P("col"),
    )
    return jax.shard_map(
        functools.partial(per_device, mesh.shape["row"], mesh.shape["col"]),
        mesh=mesh,
        in_specs=placed,
        out_specs=(P(("row", "col"), None), P(None, ("col", "row"), None), P()),
        check_vma=False,
    )
```

```python
import functools

import jax
import jax.numpy as jnp
from jax import lax
from jax.experimental import pallas as pl
from jax.experimental.pallas import tpu as pltpu
from jax.sharding import PartitionSpec as P

tiny_add = 1e-06
MESH = pl.DeviceIdType.MESH
f32, bf16 = jnp.float32, jnp.bfloat16
WHOLE_LIMIT = 64
COARSE, SLIP, SUMS, LEFT, SQUARES, BACK, ALL, COLS, PARTS, PAIR, BACK_V = range(11)


def fold(values):
    return (values * values).reshape(values.shape[0] // 8, 8, values.shape[1]).sum(axis=0)


def turn(values):
    return jnp.transpose(values.astype(f32), (1, 0))


def kernel(
    sizes,
    rows_hbm,
    cols_hbm,
    count_hbm,
    mid_rank_hbm,
    coarse_rank_hbm,
    u_hbm,
    v_hbm,
    alpha_hbm,
    near_hbm,
    mid_left_hbm,
    mid_right_hbm,
    coarse_left_hbm,
    coarse_right_hbm,
    u_out,
    v_out,
    beta_out,
    vsq_all,
    rows_smem,
    cols_smem,
    count_smem,
    mid_rank_smem,
    coarse_rank_smem,
    near,
    u_old,
    v_old,
    alpha_old,
    left,
    left_turned,
    right,
    slip,
    coarse_all,
    coarse_wide,
    begun,
    part_codes,
    weights,
    dense,
    dense_turned,
    fsend,
    frecv,
    ug,
    sq,
    bsend,
    brecv,
    vsq_col,
    v_pair,
    v_sent,
    v_back,
    spare,
    near_sem,
    in_sem,
    send_sem,
    recv_sem,
):
    n_row, n_col = sizes
    me_r, me_c = lax.axis_index("row"), lax.axis_index("col")
    slots, _, clp, clq = near.shape
    pt, rhs = u_old.shape
    pd = v_old.shape[1]
    km, kc = mid_left_hbm.shape[0], coarse_left_hbm.shape[0]
    kt = km + kc
    row_span, col_span = left.shape[1], right.shape[2]
    row_groups, col_groups = row_span // clp, col_span // clq
    per_col = clq // pd
    if n_row % 2 or per_col != 2:
        raise ValueError("uneven mesh")
    spots = row_groups * col_groups
    bunch = 8 if spots % 8 == 0 else spots
    tile = 32

    def flipped(me, mask):
        place, bit = me, 1
        while bit <= mask:
            if mask & bit:
                place = place + (1 - 2 * ((me // bit) % 2)) * bit
            bit *= 2
        return place

    if n_col & (n_col - 1):
        col_peers = [lax.rem(me_c + step, n_col) for step in range(1, n_col)]
    else:
        masks = list(range(n_col - 1, 0, -2)) + list(range(n_col - 2, 0, -2))
        col_peers = [flipped(me_c, mask) for mask in masks]
    chips = n_row // 2
    own_chip, lead = me_r // 2, lax.rem(me_r, 2)
    row_peers = []
    for step in range(1, chips):
        chip = lax.rem(own_chip + step, chips)
        row_peers += [chip * 2 + 1 - lead, chip * 2 + lead]
    row_peers += [own_chip * 2 + 1 - lead]

    loads = [
        pltpu.make_async_copy(src, dst, in_sem.at[place])
        for place, (src, dst) in enumerate(
            [
                (v_hbm, v_old),
                (coarse_right_hbm, coarse_all.at[me_r]),
                (rows_hbm, rows_smem),
                (cols_hbm, cols_smem),
                (count_hbm, count_smem),
                (mid_rank_hbm, mid_rank_smem),
                (coarse_rank_hbm, coarse_rank_smem),
                (mid_right_hbm, right),
                (mid_left_hbm, left.at[0:km, :]),
                (coarse_left_hbm, left.at[km:kt, :]),
                (u_hbm, u_old),
                (alpha_hbm, alpha_old),
            ]
        )
    ]
    loads[0].start()
    loads[1].start()

    barrier = pltpu.get_barrier_semaphore()
    for peer in col_peers:
        pl.semaphore_signal(barrier, device_id={"col": peer}, device_id_type=MESH)
    for peer in row_peers:
        pl.semaphore_signal(barrier, device_id={"row": peer}, device_id_type=MESH)
    pieces = 4 if slots % 4 == 0 else 1
    share = slots // pieces
    near_loads = [
        pltpu.make_async_copy(
            near_hbm.at[pl.ds(piece * share, share)], near.at[pl.ds(piece * share, share)], near_sem
        )
        for piece in range(pieces)
    ]
    for load in loads[2:]:
        load.start()

    def post(place, device, source, target):
        copy = pltpu.make_async_remote_copy(
            src_ref=source,
            dst_ref=target,
            send_sem=send_sem.at[place],
            recv_sem=recv_sem.at[place],
            device_id=device,
            device_id_type=MESH,
        )
        return copy

    def across_rows(place, source, target):
        for peer in row_peers:
            post(place, {"row": peer}, source(peer), target).start()

    def across_cols(place, source, target):
        for peer in col_peers:
            post(place, {"col": peer}, source(peer), target).start()

    def every(place, buffer, count):
        return post(place, {"row": row_peers[0]}, buffer.at[pl.ds(0, count - 1)], buffer.at[pl.ds(0, count - 1)])

    loads[0].wait()
    for load in near_loads:
        load.start()
    slip[me_r] = v_old[...].astype(bf16)
    loads[1].wait()
    own_codes = jnp.zeros((kc, rhs), f32)
    for k in range(3):
        own_codes = own_codes + jnp.dot(coarse_all[me_r, k], slip[me_r, k], preferred_element_type=f32)
    part_codes[me_r] = own_codes.astype(bf16)
    pl.semaphore_wait(barrier, n_row + n_col - 2)
    across_rows(PARTS, lambda peer: part_codes.at[me_r], part_codes.at[me_r])
    across_rows(SLIP, lambda peer: slip.at[me_r], slip.at[me_r])

    def pair(place, source, target):
        return post(place, {"row": own_chip * 2 + 1 - lead}, source, target)

    @pl.when(lead == 0)
    def _():
        pair(PAIR, v_old, v_pair).start()

    for load in loads[2:]:
        load.wait()
    place = lax.broadcasted_iota(jnp.int32, (kt, row_span), 0)
    limit = jnp.where(place < km, mid_rank_smem[0, 0], coarse_rank_smem[0] + km)
    left[...] = jnp.where(place < limit, left[...].astype(f32), 0.0).astype(bf16)
    spot_of = lax.broadcasted_iota(jnp.int32, (spots, rhs), 0)
    for slot in range(slots):
        spot = cols_smem[0, 0, slot] * row_groups + rows_smem[0, 0, slot]
        spot = jnp.where(slot < count_smem[0, 0], spot, -1)
        weights[slot] = jnp.where(spot_of == spot, 1.0, 0.0).astype(f32)
    for group in range(row_groups):
        span = slice(group * clp, (group + 1) * clp)
        left_turned[span, :] = turn(left[:, span]).astype(bf16)
    pltpu.make_async_copy(near_hbm, near, near_sem).wait()
    chunks = clp // tile

    sets = max(1, bunch // row_groups)
    each = bunch // sets

    def build(step, carry):
        chunk, k = step % chunks, (step // chunks) % 3
        first = step // (3 * chunks) * bunch if spots > bunch else 0
        at = pl.multiple_of(chunk * tile, tile)
        sums = [jnp.zeros((tile, clq), f32)] * bunch
        for slot in range(slots):
            block = near[slot, k, pl.ds(at, tile), :].astype(f32)
            for place in range(bunch):
                sums[place] = sums[place] + block * weights[slot, pl.ds(first + place, 1), :]
        for part in range(sets):
            places = range(part * each, (part + 1) * each)
            wide = (first + part * each) // row_groups
            groups = [(first + place) % row_groups for place in places]
            ranks = jnp.concatenate(
                [left_turned[pl.ds(pl.multiple_of(group * clp + at, tile), tile), 0:km] for group in groups], axis=0
            )
            low = jnp.dot(
                ranks, right[k, :, pl.ds(pl.multiple_of(wide * clq, clq), clq)], preferred_element_type=f32
            )
            for number, (place, group) in enumerate(zip(places, groups)):
                dense[
                    pl.ds(pl.multiple_of(group * clp + at, tile), tile),
                    pl.ds(pl.multiple_of((wide * 3 + k) * clq, clq), clq),
                ] = (sums[place] + low[number * tile : (number + 1) * tile]).astype(bf16)
        return carry

    lax.fori_loop(0, spots // bunch * 3 * chunks, build, 0)
    across_rows(COARSE, lambda peer: coarse_all.at[me_r], coarse_all.at[me_r])
    every(PARTS, part_codes, n_row).wait_recv()
    coarse_codes = jnp.zeros((kc, rhs), f32)
    for peer in range(n_row):
        coarse_codes = coarse_codes + part_codes[peer].astype(f32)
    coarse_codes = coarse_codes.astype(bf16)
    wave = min(row_span, 512)
    for group in range(row_span // wave):
        span = slice(group * wave, (group + 1) * wave)
        begun[span, :] = jnp.dot(left_turned[span, km:kt], coarse_codes, preferred_element_type=f32)
    every(SLIP, slip, n_row).wait_recv()
    gathered = jnp.concatenate(
        [
            slip[wide * per_col : (wide + 1) * per_col, k].reshape(clq, rhs)
            for wide in range(col_groups)
            for k in range(3)
        ],
        axis=0,
    )
    for group in range(row_span // wave):
        span = slice(group * wave, (group + 1) * wave)
        value = begun[span, :] + jnp.dot(dense[span, :], gathered, preferred_element_type=f32)
        fsend[group * wave // pt : (group + 1) * wave // pt] = value.astype(bf16).reshape(
            wave // pt, pt, rhs
        )
    across_cols(SUMS, lambda peer: fsend.at[peer], frecv.at[me_c])
    frecv[me_c] = fsend[me_c]

    every(COARSE, coarse_all, n_row).wait_recv()
    for peer in range(n_row):
        for k in range(3):
            coarse_wide[k, :, peer * pd : (peer + 1) * pd] = coarse_all[peer, k]

    def turn_over(step, carry):
        k, wide = step % 3, step // 3
        rank_turned = turn(coarse_wide[k, :, pl.ds(pl.multiple_of(wide * clq, clq), clq)]).astype(bf16)
        for group in range(row_groups):
            span = slice(group * clp, (group + 1) * clp)
            value = jnp.dot(rank_turned, left[km:kt, span], preferred_element_type=f32)
            value = value + turn(dense[span, pl.ds(pl.multiple_of(step * clq, clq), clq)])
            dense_turned[step, :, span] = value.astype(bf16)
        return carry

    lax.fori_loop(0, 3 * col_groups, turn_over, 0)

    every(SUMS, frecv, n_col).wait_recv()
    u_hat = -alpha_old[...] * u_old[...]
    for peer in range(n_col):
        u_hat = u_hat + frecv[peer].astype(f32)
    ug[me_c] = u_hat.astype(bf16)
    across_cols(LEFT, lambda peer: ug.at[me_c], ug.at[me_c])
    u_old[...] = u_hat
    every(LEFT, ug, n_col).wait_recv()

    gathered = ug[...].reshape(row_span, rhs)
    for step in range(chips):
        chip = lax.rem(own_chip + 1 + step, chips)
        for k in range(3):
            value = jnp.dot(dense_turned[chip * 3 + k], gathered, preferred_element_type=f32)
            value = value.astype(bf16).reshape(2, pd, rhs)
            for part in range(2):
                bsend[chip, part, k] = value[part]
        if step < chips - 1:
            post(BACK, {"row": chip * 2 + 1}, bsend.at[chip], brecv.at[me_r]).start()
        if step == 0:
            sq[me_r] = fold(gathered.astype(f32))
            across_rows(SQUARES, lambda peer: sq.at[me_r], sq.at[me_r])

    @pl.when(lead == 0)
    def _():
        pair(BACK, bsend.at[own_chip], brecv.at[me_r]).start()

    @pl.when(lead == 1)
    def _():
        brecv[me_r] = bsend[own_chip]

    every(SQUARES, sq, n_row).wait_recv()
    square_sum = jnp.zeros((8, rhs), f32)
    for peer in range(n_row):
        square_sum = square_sum + sq[peer]
    points = pt * n_row * n_col
    beta = jnp.sqrt(jnp.sum(square_sum, axis=0, keepdims=True) / points + tiny_add)
    beta_out[...] = beta
    inverse = 1.0 / beta
    u_out[...] = u_old[...] * inverse
    whole = n_row * n_col <= WHOLE_LIMIT
    leads = vsq_all.shape[0]

    @pl.when(lead == 1)
    def _():
        pair(PAIR, v_pair, v_pair).wait_recv()
        every(BACK, brecv, n_row).wait_recv()
        v_squares = jnp.zeros((8, rhs), f32)
        for part, (old, new) in enumerate([(v_pair, v_sent), (v_old, v_out)]):
            for k in range(3):
                total = jnp.zeros((pd, rhs), f32)
                for peer in range(n_row):
                    total = total + brecv[peer, part, k].astype(f32)
                v_hat = total * inverse - beta * old[k]
                new[k] = v_hat
                v_squares = v_squares + fold(v_hat)
        if whole:
            own = vsq_all.at[me_c * chips + own_chip]
            vsq_all[me_c * chips + own_chip] = jnp.sum(v_squares, axis=0, keepdims=True)
            others = [(a, b) for b in reversed(range(n_col)) for a in reversed(range(n_row))][:-1]
            for a, b in others:
                post(ALL, (lax.rem(me_r + a, n_row), lax.rem(me_c + b, n_col)), own, own).start()
        else:
            vsq_col[me_c] = v_squares
            across_cols(COLS, lambda peer: vsq_col.at[me_c], vsq_col.at[me_c])
            every(COLS, vsq_col, n_col).wait_recv()
            v_squares = jnp.zeros((8, rhs), f32)
            for peer in range(n_col):
                v_squares = v_squares + vsq_col[peer]
            vsq_all[own_chip] = v_squares
            across_rows(ALL, lambda peer: vsq_all.at[own_chip], vsq_all.at[own_chip])
            every(COLS, vsq_col, n_col).wait_send()
        pair(BACK_V, v_sent, v_back).start()
        every(ALL, vsq_all, leads).wait_recv()
        every(BACK, bsend, chips).wait_send()
        pair(BACK_V, v_sent, v_back).wait_send()
        every(ALL, spare, spare.shape[0]).wait_send()

    @pl.when(lead == 0)
    def _():
        pair(BACK_V, v_back, v_back).wait_recv()
        v_out[...] = v_back[...]
        every(ALL, vsq_all, leads + 1).wait_recv()
        pair(PAIR, v_old, v_pair).wait_send()
        every(BACK, bsend, chips + 1).wait_send()

    for place, buffer in (
        (PARTS, part_codes),
        (COARSE, coarse_all),
        (SLIP, slip),
        (SUMS, fsend),
        (LEFT, ug),
        (SQUARES, sq),
    ):
        every(place, buffer, buffer.shape[0]).wait_send()


def finish(unknowns, u_ref, v_ref, beta_ref, squares_ref, u_out, v_out, norms_out):
    total = jnp.zeros(squares_ref.shape[1:], f32)
    for peer in range(squares_ref.shape[0]):
        total = total + squares_ref[peer]
    alpha = jnp.sqrt(jnp.sum(total, axis=0, keepdims=True) / unknowns + tiny_add)
    norms_out[0:1, :] = beta_ref[...]
    norms_out[1:2, :] = alpha
    u_out[...] = u_ref[...]
    v_out[...] = v_ref[...] / alpha


def per_device(
    n_row,
    n_col,
    u_state,
    v_state,
    alpha_prev,
    near_blocks,
    near_rows,
    near_cols,
    near_count,
    mid_left,
    mid_right,
    mid_rank,
    coarse_left,
    coarse_right,
    coarse_rank,
):
    slots, clp, _, clq = near_blocks.shape[2:]
    pt, rhs = u_state.shape
    pd = v_state.shape[1]
    km, kc = mid_left.shape[1], coarse_left.shape[1]
    kt = km + kc
    row_span, col_span = mid_left.shape[2], mid_right.shape[3]
    row_groups, col_groups = row_span // clp, col_span // clq
    in_hbm = pl.BlockSpec(memory_space=pltpu.HBM)
    vmem = pl.BlockSpec(memory_space=pltpu.VMEM)
    dma = pltpu.SemaphoreType.DMA
    whole = n_row * n_col <= WHOLE_LIMIT
    sums = (n_row // 2 * n_col, 1, rhs) if whole else (n_row // 2, 8, rhs)
    scratch = [
        pltpu.SMEM(near_rows.shape, jnp.int32),
        pltpu.SMEM(near_cols.shape, jnp.int32),
        pltpu.SMEM(near_count.shape, jnp.int32),
        pltpu.SMEM(mid_rank.shape, jnp.int32),
        pltpu.SMEM(coarse_rank.shape, jnp.int32),
        pltpu.VMEM((slots, 3, clp, clq), bf16),
        pltpu.VMEM((pt, rhs), f32),
        pltpu.VMEM((3, pd, rhs), f32),
        pltpu.VMEM((1, rhs), f32),
        pltpu.VMEM((kt, row_span), bf16),
        pltpu.VMEM((row_span, kt), bf16),
        pltpu.VMEM((3, km, col_span), bf16),
        pltpu.VMEM((n_row, 3, pd, rhs), bf16),
        pltpu.VMEM((n_row, 3, kc, pd), bf16),
        pltpu.VMEM((3, kc, col_span), bf16),
        pltpu.VMEM((row_span, rhs), f32),
        pltpu.VMEM((n_row, kc, rhs), bf16),
        pltpu.VMEM((slots, row_groups * col_groups, rhs), f32),
        pltpu.VMEM((row_span, 3 * col_span), bf16),
        pltpu.VMEM((3 * col_groups, clq, row_span), bf16),
        pltpu.VMEM((n_col, pt, rhs), bf16),
        pltpu.VMEM((n_col, pt, rhs), bf16),
        pltpu.VMEM((n_col, pt, rhs), bf16),
        pltpu.VMEM((n_row, 8, rhs), f32),
        pltpu.VMEM((n_row // 2, 2, 3, pd, rhs), bf16),
        pltpu.VMEM((n_row, 2, 3, pd, rhs), bf16),
        pltpu.VMEM((n_col, 8, rhs), f32),
        pltpu.VMEM((3, pd, rhs), f32),
        pltpu.VMEM((3, pd, rhs), f32),
        pltpu.VMEM((3, pd, rhs), f32),
        pltpu.VMEM((n_row * n_col, 1, rhs) if whole else (n_row, 8, rhs), f32),
        dma,
        dma((12,)),
        dma((11,)),
        dma((11,)),
    ]
    held = pl.pallas_call(
        functools.partial(kernel, (n_row, n_col)),
        out_shape=(
            pltpu.VMEM((pt, rhs), f32),
            pltpu.VMEM((3, pd, rhs), f32),
            pltpu.VMEM((1, rhs), f32),
            pltpu.VMEM(sums, f32),
        ),
        in_specs=[in_hbm] * 13,
        out_specs=(vmem,) * 4,
        scratch_shapes=scratch,
        compiler_params=pltpu.CompilerParams(
            collective_id=0, has_side_effects=True, vmem_limit_bytes=60 * 1024 * 1024
        ),
        name="lsqr",
    )(
        near_rows,
        near_cols,
        near_count,
        mid_rank,
        coarse_rank,
        u_state,
        v_state,
        alpha_prev.reshape(1, rhs),
        jnp.transpose(near_blocks[0, 0], (0, 2, 1, 3)),
        mid_left[0],
        jnp.transpose(mid_right[0], (1, 0, 2)),
        coarse_left[0],
        jnp.transpose(coarse_right, (1, 0, 2)),
    )
    return pl.pallas_call(
        functools.partial(finish, 3 * pd * n_row * n_col),
        out_shape=(
            jax.ShapeDtypeStruct((pt, rhs), f32),
            jax.ShapeDtypeStruct((3, pd, rhs), f32),
            jax.ShapeDtypeStruct((2, rhs), f32),
        ),
        in_specs=[vmem] * 4,
        out_specs=(vmem,) * 3,
        name="finish",
    )(*[pltpu.with_memory_space_constraint(value, pltpu.VMEM) for value in held])


def solution(mesh):
    placed = (
        P(("row", "col"), None),
        P(None, ("col", "row"), None),
        P(),
        P("row", "col", None, None, None, None),
        P("row", "col", None),
        P("row", "col", None),
        P("row", "col"),
        P("col", None, "row"),
        P("row", None, None, "col"),
        P("row", "col"),
        P("col", None, "row"),
        P(None, None, ("col", "row")),
        P("col"),
    )
    return jax.shard_map(
        functools.partial(per_device, mesh.shape["row"], mesh.shape["col"]),
        mesh=mesh,
        in_specs=placed,
        out_specs=(P(("row", "col"), None), P(None, ("col", "row"), None), P()),
        check_vma=False,
    )
```

```python
import functools

import jax
import jax.numpy as jnp
from jax import lax
from jax.experimental import pallas as pl
from jax.experimental.pallas import tpu as pltpu
from jax.sharding import PartitionSpec as P

tiny_add = 1e-06
MESH = pl.DeviceIdType.MESH
f32, bf16 = jnp.float32, jnp.bfloat16
WHOLE_LIMIT = 64
COARSE, SLIP, SUMS, LEFT, SQUARES, BACK, ALL, COLS, PARTS, PAIR, BACK_V = range(11)


def fold(values):
    return (values * values).reshape(values.shape[0] // 8, 8, values.shape[1]).sum(axis=0)


def turn(values):
    return jnp.transpose(values.astype(f32), (1, 0))


def kernel(
    sizes,
    rows_hbm,
    cols_hbm,
    count_hbm,
    mid_rank_hbm,
    coarse_rank_hbm,
    u_hbm,
    v_hbm,
    alpha_hbm,
    near_hbm,
    mid_left_hbm,
    mid_right_hbm,
    coarse_left_hbm,
    coarse_right_hbm,
    u_out,
    v_out,
    beta_out,
    vsq_all,
    rows_smem,
    cols_smem,
    count_smem,
    mid_rank_smem,
    coarse_rank_smem,
    near,
    u_old,
    v_old,
    alpha_old,
    left,
    left_turned,
    right,
    slip,
    coarse_all,
    coarse_wide,
    begun,
    part_codes,
    weights,
    dense,
    dense_turned,
    fsend,
    frecv,
    ug,
    sq,
    bsend,
    brecv,
    vsq_col,
    v_pair,
    v_sent,
    v_back,
    spare,
    near_sem,
    in_sem,
    send_sem,
    recv_sem,
    known,
):
    n_row, n_col = sizes
    me_r, me_c = lax.axis_index("row"), lax.axis_index("col")
    slots, _, clp, clq = near.shape
    pt, rhs = u_old.shape
    pd = v_old.shape[1]
    km, kc = mid_left_hbm.shape[0], coarse_left_hbm.shape[0]
    kt = km + kc
    row_span, col_span = left.shape[1], right.shape[2]
    row_groups, col_groups = row_span // clp, col_span // clq
    per_col = clq // pd
    if n_row % 2 or per_col != 2:
        raise ValueError("uneven mesh")
    spots = row_groups * col_groups
    bunch = 8 if spots % 8 == 0 else spots
    tile = 32

    def flipped(me, mask):
        place, bit = me, 1
        while bit <= mask:
            if mask & bit:
                place = place + (1 - 2 * ((me // bit) % 2)) * bit
            bit *= 2
        return place

    if n_col & (n_col - 1):
        col_peers = [lax.rem(me_c + step, n_col) for step in range(1, n_col)]
    else:
        masks = list(range(n_col - 1, 0, -2)) + list(range(n_col - 2, 0, -2))
        col_peers = [flipped(me_c, mask) for mask in masks]
    far_cols = col_peers
    if not n_col & (n_col - 1):
        far_cols = [flipped(me_c, mask) for mask in range(n_col - 1, 0, -1)]
    chips = n_row // 2
    own_chip, lead = me_r // 2, lax.rem(me_r, 2)
    row_peers = []
    for step in range(1, chips):
        chip = lax.rem(own_chip + step, chips)
        row_peers += [chip * 2 + 1 - lead, chip * 2 + lead]
    row_peers += [own_chip * 2 + 1 - lead]

    loads = [
        pltpu.make_async_copy(src, dst, in_sem.at[place])
        for place, (src, dst) in enumerate(
            [
                (v_hbm, v_old),
                (coarse_right_hbm, coarse_all.at[me_r]),
                (rows_hbm, rows_smem),
                (cols_hbm, cols_smem),
                (count_hbm, count_smem),
                (mid_rank_hbm, mid_rank_smem),
                (coarse_rank_hbm, coarse_rank_smem),
                (mid_right_hbm, right),
                (mid_left_hbm, left.at[0:km, :]),
                (coarse_left_hbm, left.at[km:kt, :]),
                (u_hbm, u_old),
                (alpha_hbm, alpha_old),
            ]
        )
    ]
    loads[0].start()
    loads[1].start()

    barrier = pltpu.get_barrier_semaphore()
    @pl.when(lead == 1)
    def _():
        for peer in col_peers:
            pl.semaphore_signal(barrier, device_id={"col": peer}, device_id_type=MESH)

    for peer in row_peers:
        pl.semaphore_signal(barrier, device_id={"row": peer}, device_id_type=MESH)
    pieces = 4 if slots % 4 == 0 else 1
    share = slots // pieces
    near_loads = [
        pltpu.make_async_copy(
            near_hbm.at[pl.ds(piece * share, share)], near.at[pl.ds(piece * share, share)], near_sem
        )
        for piece in range(pieces)
    ]
    for load in loads[2:]:
        load.start()

    def post(place, device, source, target):
        copy = pltpu.make_async_remote_copy(
            src_ref=source,
            dst_ref=target,
            send_sem=send_sem.at[place],
            recv_sem=recv_sem.at[place],
            device_id=device,
            device_id_type=MESH,
        )
        return copy

    def across_rows(place, source, target):
        for peer in row_peers:
            post(place, {"row": peer}, source(peer), target).start()

    def across_cols(place, source, target):
        for peer in col_peers:
            post(place, {"col": peer}, source(peer), target).start()

    def every(place, buffer, count):
        return post(place, {"row": row_peers[0]}, buffer.at[pl.ds(0, count - 1)], buffer.at[pl.ds(0, count - 1)])

    loads[0].wait()
    for load in near_loads:
        load.start()
    slip[me_r] = v_old[...].astype(bf16)
    loads[1].wait()
    own_codes = jnp.zeros((kc, rhs), f32)
    for k in range(3):
        own_codes = own_codes + jnp.dot(coarse_all[me_r, k], slip[me_r, k], preferred_element_type=f32)
    part_codes[me_r] = own_codes.astype(bf16)
    pl.semaphore_wait(barrier, n_row - 1 + lead * (n_col - 1))
    across_rows(PARTS, lambda peer: part_codes.at[me_r], part_codes.at[me_r])
    across_rows(SLIP, lambda peer: slip.at[me_r], slip.at[me_r])

    def pair(place, source, target):
        return post(place, {"row": own_chip * 2 + 1 - lead}, source, target)

    @pl.when(lead == 0)
    def _():
        pair(PAIR, v_old, v_pair).start()

    @pl.when(lead == 1)
    def _():
        for peer in col_peers:
            pl.semaphore_signal(known, device_id={"col": peer}, device_id_type=MESH)

    for load in loads[2:]:
        load.wait()
    place = lax.broadcasted_iota(jnp.int32, (kt, row_span), 0)
    limit = jnp.where(place < km, mid_rank_smem[0, 0], coarse_rank_smem[0] + km)
    left[...] = jnp.where(place < limit, left[...].astype(f32), 0.0).astype(bf16)
    spot_of = lax.broadcasted_iota(jnp.int32, (spots, rhs), 0)
    for slot in range(slots):
        spot = cols_smem[0, 0, slot] * row_groups + rows_smem[0, 0, slot]
        spot = jnp.where(slot < count_smem[0, 0], spot, -1)
        weights[slot] = jnp.where(spot_of == spot, 1.0, 0.0).astype(f32)
    for group in range(row_groups):
        span = slice(group * clp, (group + 1) * clp)
        left_turned[span, :] = turn(left[:, span]).astype(bf16)
    pltpu.make_async_copy(near_hbm, near, near_sem).wait()
    chunks = clp // tile

    sets = max(1, bunch // row_groups)
    each = bunch // sets

    def build(step, carry):
        chunk, k = step % chunks, (step // chunks) % 3
        first = step // (3 * chunks) * bunch if spots > bunch else 0
        at = pl.multiple_of(chunk * tile, tile)
        sums = [jnp.zeros((tile, clq), f32)] * bunch
        for slot in range(slots):
            block = near[slot, k, pl.ds(at, tile), :].astype(f32)
            for place in range(bunch):
                sums[place] = sums[place] + block * weights[slot, pl.ds(first + place, 1), :]
        for part in range(sets):
            places = range(part * each, (part + 1) * each)
            wide = (first + part * each) // row_groups
            groups = [(first + place) % row_groups for place in places]
            ranks = jnp.concatenate(
                [left_turned[pl.ds(pl.multiple_of(group * clp + at, tile), tile), 0:km] for group in groups], axis=0
            )
            low = jnp.dot(
                ranks, right[k, :, pl.ds(pl.multiple_of(wide * clq, clq), clq)], preferred_element_type=f32
            )
            for number, (place, group) in enumerate(zip(places, groups)):
                dense[
                    pl.ds(pl.multiple_of(group * clp + at, tile), tile),
                    pl.ds(pl.multiple_of((wide * 3 + k) * clq, clq), clq),
                ] = (sums[place] + low[number * tile : (number + 1) * tile]).astype(bf16)
        return carry

    lax.fori_loop(0, spots // bunch * 3 * chunks, build, 0)

    @pl.when(lead == 1)
    def _():
        pl.semaphore_wait(known, n_col - 1)
        pl.semaphore_signal(known, device_id={"row": me_r - 1}, device_id_type=MESH)

    across_rows(COARSE, lambda peer: coarse_all.at[me_r], coarse_all.at[me_r])
    every(PARTS, part_codes, n_row).wait_recv()
    coarse_codes = jnp.zeros((kc, rhs), f32)
    for peer in range(n_row):
        coarse_codes = coarse_codes + part_codes[peer].astype(f32)
    coarse_codes = coarse_codes.astype(bf16)
    wave = min(row_span, 512)
    for group in range(row_span // wave):
        span = slice(group * wave, (group + 1) * wave)
        begun[span, :] = jnp.dot(left_turned[span, km:kt], coarse_codes, preferred_element_type=f32)
    every(SLIP, slip, n_row).wait_recv()
    gathered = jnp.concatenate(
        [
            slip[wide * per_col : (wide + 1) * per_col, k].reshape(clq, rhs)
            for wide in range(col_groups)
            for k in range(3)
        ],
        axis=0,
    )
    for group in range(row_span // wave):
        span = slice(group * wave, (group + 1) * wave)
        value = begun[span, :] + jnp.dot(dense[span, :], gathered, preferred_element_type=f32)
        fsend[group * wave // pt : (group + 1) * wave // pt] = value.astype(bf16).reshape(
            wave // pt, pt, rhs
        )
    @pl.when(lead == 0)
    def _():
        pl.semaphore_wait(known, 1)

    across_cols(SUMS, lambda peer: fsend.at[peer], frecv.at[me_c])
    frecv[me_c] = fsend[me_c]

    every(COARSE, coarse_all, n_row).wait_recv()
    for peer in range(n_row):
        for k in range(3):
            coarse_wide[k, :, peer * pd : (peer + 1) * pd] = coarse_all[peer, k]

    def turn_over(step, carry):
        k, wide = step % 3, step // 3
        rank_turned = turn(coarse_wide[k, :, pl.ds(pl.multiple_of(wide * clq, clq), clq)]).astype(bf16)
        for group in range(row_groups):
            span = slice(group * clp, (group + 1) * clp)
            value = jnp.dot(rank_turned, left[km:kt, span], preferred_element_type=f32)
            value = value + turn(dense[span, pl.ds(pl.multiple_of(step * clq, clq), clq)])
            dense_turned[step, :, span] = value.astype(bf16)
        return carry

    lax.fori_loop(0, 3 * col_groups, turn_over, 0)

    every(SUMS, frecv, n_col).wait_recv()
    u_hat = -alpha_old[...] * u_old[...]
    for peer in range(n_col):
        u_hat = u_hat + frecv[peer].astype(f32)
    ug[me_c] = u_hat.astype(bf16)
    across_cols(LEFT, lambda peer: ug.at[me_c], ug.at[me_c])
    u_old[...] = u_hat
    every(LEFT, ug, n_col).wait_recv()

    gathered = ug[...].reshape(row_span, rhs)
    for step in range(chips):
        chip = lax.rem(own_chip + 1 + step, chips)
        for k in range(3):
            value = jnp.dot(dense_turned[chip * 3 + k], gathered, preferred_element_type=f32)
            value = value.astype(bf16).reshape(2, pd, rhs)
            for part in range(2):
                bsend[chip, part, k] = value[part]
        if step < chips - 1:
            post(BACK, {"row": chip * 2 + 1}, bsend.at[chip], brecv.at[me_r]).start()
        if step == 0:
            sq[me_r] = fold(gathered.astype(f32))
            across_rows(SQUARES, lambda peer: sq.at[me_r], sq.at[me_r])

    @pl.when(lead == 0)
    def _():
        pair(BACK, bsend.at[own_chip], brecv.at[me_r]).start()

    @pl.when(lead == 1)
    def _():
        brecv[me_r] = bsend[own_chip]

    every(SQUARES, sq, n_row).wait_recv()
    square_sum = jnp.zeros((8, rhs), f32)
    for peer in range(n_row):
        square_sum = square_sum + sq[peer]
    points = pt * n_row * n_col
    beta = jnp.sqrt(jnp.sum(square_sum, axis=0, keepdims=True) / points + tiny_add)
    beta_out[...] = beta
    inverse = 1.0 / beta
    u_out[...] = u_old[...] * inverse
    def sent():
        for place, buffer in (
            (PARTS, part_codes),
            (COARSE, coarse_all),
            (SLIP, slip),
            (SUMS, fsend),
            (LEFT, ug),
            (SQUARES, sq),
        ):
            every(place, buffer, buffer.shape[0]).wait_send()

    whole = n_row * n_col <= WHOLE_LIMIT
    leads = vsq_all.shape[0]

    @pl.when(lead == 1)
    def _():
        pair(PAIR, v_pair, v_pair).wait_recv()
        every(BACK, brecv, n_row).wait_recv()
        v_squares = jnp.zeros((8, rhs), f32)
        for part, (old, new) in enumerate([(v_pair, v_sent), (v_old, v_out)]):
            for k in range(3):
                total = jnp.zeros((pd, rhs), f32)
                for peer in range(n_row):
                    total = total + brecv[peer, part, k].astype(f32)
                v_hat = total * inverse - beta * old[k]
                new[k] = v_hat
                v_squares = v_squares + fold(v_hat)
        if whole:
            own = vsq_all.at[me_c * chips + own_chip]
            vsq_all[me_c * chips + own_chip] = jnp.sum(v_squares, axis=0, keepdims=True)
            for col in far_cols + [me_c]:
                for row in row_peers + ([] if col is me_c else [me_r]):
                    post(ALL, (row, col), own, own).start()
        else:
            vsq_col[me_c] = v_squares
            across_cols(COLS, lambda peer: vsq_col.at[me_c], vsq_col.at[me_c])
            every(COLS, vsq_col, n_col).wait_recv()
            v_squares = jnp.zeros((8, rhs), f32)
            for peer in range(n_col):
                v_squares = v_squares + vsq_col[peer]
            vsq_all[own_chip] = v_squares
            across_rows(ALL, lambda peer: vsq_all.at[own_chip], vsq_all.at[own_chip])
            every(COLS, vsq_col, n_col).wait_send()
        pair(BACK_V, v_sent, v_back).start()
        every(BACK, bsend, chips).wait_send()
        sent()
        pair(BACK_V, v_sent, v_back).wait_send()
        every(ALL, spare, spare.shape[0]).wait_send()
        every(ALL, vsq_all, leads).wait_recv()

    @pl.when(lead == 0)
    def _():
        pair(BACK_V, v_back, v_back).wait_recv()
        v_out[...] = v_back[...]
        pair(PAIR, v_old, v_pair).wait_send()
        every(BACK, bsend, chips + 1).wait_send()
        sent()
        every(ALL, vsq_all, leads + 1).wait_recv()


def finish(unknowns, u_ref, v_ref, beta_ref, squares_ref, u_out, v_out, norms_out):
    total = jnp.zeros(squares_ref.shape[1:], f32)
    for peer in range(squares_ref.shape[0]):
        total = total + squares_ref[peer]
    alpha = jnp.sqrt(jnp.sum(total, axis=0, keepdims=True) / unknowns + tiny_add)
    norms_out[0:1, :] = beta_ref[...]
    norms_out[1:2, :] = alpha
    u_out[...] = u_ref[...]
    v_out[...] = v_ref[...] / alpha


def per_device(
    n_row,
    n_col,
    u_state,
    v_state,
    alpha_prev,
    near_blocks,
    near_rows,
    near_cols,
    near_count,
    mid_left,
    mid_right,
    mid_rank,
    coarse_left,
    coarse_right,
    coarse_rank,
):
    slots, clp, _, clq = near_blocks.shape[2:]
    pt, rhs = u_state.shape
    pd = v_state.shape[1]
    km, kc = mid_left.shape[1], coarse_left.shape[1]
    kt = km + kc
    row_span, col_span = mid_left.shape[2], mid_right.shape[3]
    row_groups, col_groups = row_span // clp, col_span // clq
    in_hbm = pl.BlockSpec(memory_space=pltpu.HBM)
    vmem = pl.BlockSpec(memory_space=pltpu.VMEM)
    dma = pltpu.SemaphoreType.DMA
    whole = n_row * n_col <= WHOLE_LIMIT
    sums = (n_row // 2 * n_col, 1, rhs) if whole else (n_row // 2, 8, rhs)
    scratch = [
        pltpu.SMEM(near_rows.shape, jnp.int32),
        pltpu.SMEM(near_cols.shape, jnp.int32),
        pltpu.SMEM(near_count.shape, jnp.int32),
        pltpu.SMEM(mid_rank.shape, jnp.int32),
        pltpu.SMEM(coarse_rank.shape, jnp.int32),
        pltpu.VMEM((slots, 3, clp, clq), bf16),
        pltpu.VMEM((pt, rhs), f32),
        pltpu.VMEM((3, pd, rhs), f32),
        pltpu.VMEM((1, rhs), f32),
        pltpu.VMEM((kt, row_span), bf16),
        pltpu.VMEM((row_span, kt), bf16),
        pltpu.VMEM((3, km, col_span), bf16),
        pltpu.VMEM((n_row, 3, pd, rhs), bf16),
        pltpu.VMEM((n_row, 3, kc, pd), bf16),
        pltpu.VMEM((3, kc, col_span), bf16),
        pltpu.VMEM((row_span, rhs), f32),
        pltpu.VMEM((n_row, kc, rhs), bf16),
        pltpu.VMEM((slots, row_groups * col_groups, rhs), f32),
        pltpu.VMEM((row_span, 3 * col_span), bf16),
        pltpu.VMEM((3 * col_groups, clq, row_span), bf16),
        pltpu.VMEM((n_col, pt, rhs), bf16),
        pltpu.VMEM((n_col, pt, rhs), bf16),
        pltpu.VMEM((n_col, pt, rhs), bf16),
        pltpu.VMEM((n_row, 8, rhs), f32),
        pltpu.VMEM((n_row // 2, 2, 3, pd, rhs), bf16),
        pltpu.VMEM((n_row, 2, 3, pd, rhs), bf16),
        pltpu.VMEM((n_col, 8, rhs), f32),
        pltpu.VMEM((3, pd, rhs), f32),
        pltpu.VMEM((3, pd, rhs), f32),
        pltpu.VMEM((3, pd, rhs), f32),
        pltpu.VMEM((n_row * n_col, 1, rhs) if whole else (n_row, 8, rhs), f32),
        dma,
        dma((12,)),
        dma((11,)),
        dma((11,)),
        pltpu.SemaphoreType.REGULAR,
    ]
    held = pl.pallas_call(
        functools.partial(kernel, (n_row, n_col)),
        out_shape=(
            pltpu.VMEM((pt, rhs), f32),
            pltpu.VMEM((3, pd, rhs), f32),
            pltpu.VMEM((1, rhs), f32),
            pltpu.VMEM(sums, f32),
        ),
        in_specs=[in_hbm] * 13,
        out_specs=(vmem,) * 4,
        scratch_shapes=scratch,
        compiler_params=pltpu.CompilerParams(
            collective_id=0, has_side_effects=True, vmem_limit_bytes=60 * 1024 * 1024
        ),
        name="lsqr",
    )(
        near_rows,
        near_cols,
        near_count,
        mid_rank,
        coarse_rank,
        u_state,
        v_state,
        alpha_prev.reshape(1, rhs),
        jnp.transpose(near_blocks[0, 0], (0, 2, 1, 3)),
        mid_left[0],
        jnp.transpose(mid_right[0], (1, 0, 2)),
        coarse_left[0],
        jnp.transpose(coarse_right, (1, 0, 2)),
    )
    return pl.pallas_call(
        functools.partial(finish, 3 * pd * n_row * n_col),
        out_shape=(
            jax.ShapeDtypeStruct((pt, rhs), f32),
            jax.ShapeDtypeStruct((3, pd, rhs), f32),
            jax.ShapeDtypeStruct((2, rhs), f32),
        ),
        in_specs=[vmem] * 4,
        out_specs=(vmem,) * 3,
        name="finish",
    )(*[pltpu.with_memory_space_constraint(value, pltpu.VMEM) for value in held])


def solution(mesh):
    placed = (
        P(("row", "col"), None),
        P(None, ("col", "row"), None),
        P(),
        P("row", "col", None, None, None, None),
        P("row", "col", None),
        P("row", "col", None),
        P("row", "col"),
        P("col", None, "row"),
        P("row", None, None, "col"),
        P("row", "col"),
        P("col", None, "row"),
        P(None, None, ("col", "row")),
        P("col"),
    )
    return jax.shard_map(
        functools.partial(per_device, mesh.shape["row"], mesh.shape["col"]),
        mesh=mesh,
        in_specs=placed,
        out_specs=(P(("row", "col"), None), P(None, ("col", "row"), None), P()),
        check_vma=False,
    )
```

```python
import functools

import jax
import jax.numpy as jnp
from jax import lax
from jax.experimental import pallas as pl
from jax.experimental.pallas import tpu as pltpu
from jax.sharding import PartitionSpec as P

tiny_add = 1e-06
MESH = pl.DeviceIdType.MESH
f32, bf16 = jnp.float32, jnp.bfloat16
WHOLE_LIMIT = 64
COARSE, SLIP, SUMS, LEFT, SQUARES, BACK, ALL, COLS, PARTS, PAIR, BACK_V, SLIP_NEAR = range(12)


def fold(values):
    return (values * values).reshape(values.shape[0] // 8, 8, values.shape[1]).sum(axis=0)


def turn(values):
    return jnp.transpose(values.astype(f32), (1, 0))


def kernel(
    sizes,
    rows_hbm,
    cols_hbm,
    count_hbm,
    mid_rank_hbm,
    coarse_rank_hbm,
    u_hbm,
    v_hbm,
    alpha_hbm,
    near_hbm,
    mid_left_hbm,
    mid_right_hbm,
    coarse_left_hbm,
    coarse_right_hbm,
    u_out,
    v_out,
    beta_out,
    vsq_all,
    rows_smem,
    cols_smem,
    count_smem,
    mid_rank_smem,
    coarse_rank_smem,
    near,
    u_old,
    v_old,
    alpha_old,
    left,
    left_turned,
    right,
    slip,
    coarse_all,
    coarse_wide,
    begun,
    part_codes,
    weights,
    dense,
    dense_turned,
    fsend,
    frecv,
    ug,
    sq,
    bsend,
    brecv,
    vsq_col,
    v_pair,
    v_sent,
    v_back,
    spare,
    near_sem,
    in_sem,
    send_sem,
    recv_sem,
    known,
):
    n_row, n_col = sizes
    me_r, me_c = lax.axis_index("row"), lax.axis_index("col")
    slots, _, clp, clq = near.shape
    pt, rhs = u_old.shape
    pd = v_old.shape[1]
    km, kc = mid_left_hbm.shape[0], coarse_left_hbm.shape[0]
    kt = km + kc
    row_span, col_span = left.shape[1], right.shape[2]
    row_groups, col_groups = row_span // clp, col_span // clq
    per_col = clq // pd
    if n_row % 2 or per_col != 2:
        raise ValueError("uneven mesh")
    spots = row_groups * col_groups
    bunch = 8 if spots % 8 == 0 else spots
    tile = 32

    def flipped(me, mask):
        place, bit = me, 1
        while bit <= mask:
            if mask & bit:
                place = place + (1 - 2 * ((me // bit) % 2)) * bit
            bit *= 2
        return place

    if n_col & (n_col - 1):
        col_peers = [lax.rem(me_c + step, n_col) for step in range(1, n_col)]
    else:
        masks = list(range(n_col - 1, 0, -2)) + list(range(n_col - 2, 0, -2))
        col_peers = [flipped(me_c, mask) for mask in masks]
    far_cols = col_peers
    if not n_col & (n_col - 1):
        far_cols = [flipped(me_c, mask) for mask in range(n_col - 1, 0, -1)]
    chips = n_row // 2
    own_chip, lead = me_r // 2, lax.rem(me_r, 2)
    row_peers = []
    for step in range(1, chips):
        chip = lax.rem(own_chip + step, chips)
        row_peers += [chip * 2 + 1 - lead, chip * 2 + lead]
    row_peers += [own_chip * 2 + 1 - lead]

    loads = [
        pltpu.make_async_copy(src, dst, in_sem.at[place])
        for place, (src, dst) in enumerate(
            [
                (v_hbm, v_old),
                (coarse_right_hbm, coarse_all.at[me_r]),
                (rows_hbm, rows_smem),
                (cols_hbm, cols_smem),
                (count_hbm, count_smem),
                (mid_rank_hbm, mid_rank_smem),
                (coarse_rank_hbm, coarse_rank_smem),
                (mid_right_hbm, right),
                (mid_left_hbm, left.at[0:km, :]),
                (coarse_left_hbm, left.at[km:kt, :]),
                (u_hbm, u_old),
                (alpha_hbm, alpha_old),
            ]
        )
    ]
    loads[0].start()
    loads[1].start()

    barrier = pltpu.get_barrier_semaphore()
    @pl.when(lead == 1)
    def _():
        for peer in col_peers:
            pl.semaphore_signal(barrier, device_id={"col": peer}, device_id_type=MESH)

    for peer in row_peers:
        pl.semaphore_signal(barrier, device_id={"row": peer}, device_id_type=MESH)
    pieces = 4 if slots % 4 == 0 else 1
    share = slots // pieces
    near_loads = [
        pltpu.make_async_copy(
            near_hbm.at[pl.ds(piece * share, share)], near.at[pl.ds(piece * share, share)], near_sem
        )
        for piece in range(pieces)
    ]
    for load in loads[2:]:
        load.start()

    def post(place, device, source, target):
        copy = pltpu.make_async_remote_copy(
            src_ref=source,
            dst_ref=target,
            send_sem=send_sem.at[place],
            recv_sem=recv_sem.at[place],
            device_id=device,
            device_id_type=MESH,
        )
        return copy

    def across_rows(place, source, target):
        for peer in row_peers:
            post(place, {"row": peer}, source(peer), target).start()

    def across_cols(place, source, target):
        for peer in col_peers:
            post(place, {"col": peer}, source(peer), target).start()

    def every(place, buffer, count):
        return post(place, {"row": row_peers[0]}, buffer.at[pl.ds(0, count - 1)], buffer.at[pl.ds(0, count - 1)])

    loads[0].wait()
    for load in near_loads:
        load.start()
    slip[me_r] = v_old[...].astype(bf16)
    loads[1].wait()
    own_codes = jnp.zeros((kc, rhs), f32)
    for k in range(3):
        own_codes = own_codes + jnp.dot(coarse_all[me_r, k], slip[me_r, k], preferred_element_type=f32)
    part_codes[me_r] = own_codes.astype(bf16)
    pl.semaphore_wait(barrier, n_row - 1 + lead * (n_col - 1))
    across_rows(PARTS, lambda peer: part_codes.at[me_r], part_codes.at[me_r])
    for peer in row_peers[:-1]:
        post(SLIP, {"row": peer}, slip.at[me_r], slip.at[me_r]).start()

    def pair(place, source, target):
        return post(place, {"row": own_chip * 2 + 1 - lead}, source, target)

    pair(SLIP_NEAR, slip.at[me_r], slip.at[me_r]).start()

    @pl.when(lead == 0)
    def _():
        pair(PAIR, v_old, v_pair).start()

    @pl.when(lead == 1)
    def _():
        for peer in col_peers:
            pl.semaphore_signal(known, device_id={"col": peer}, device_id_type=MESH)

    for load in loads[2:]:
        load.wait()
    place = lax.broadcasted_iota(jnp.int32, (kt, row_span), 0)
    limit = jnp.where(place < km, mid_rank_smem[0, 0], coarse_rank_smem[0] + km)
    left[...] = jnp.where(place < limit, left[...].astype(f32), 0.0).astype(bf16)
    spot_of = lax.broadcasted_iota(jnp.int32, (spots, rhs), 0)
    for slot in range(slots):
        spot = cols_smem[0, 0, slot] * row_groups + rows_smem[0, 0, slot]
        spot = jnp.where(slot < count_smem[0, 0], spot, -1)
        weights[slot] = jnp.where(spot_of == spot, 1.0, 0.0).astype(f32)
    for group in range(row_groups):
        span = slice(group * clp, (group + 1) * clp)
        left_turned[span, :] = turn(left[:, span]).astype(bf16)
    pltpu.make_async_copy(near_hbm, near, near_sem).wait()
    chunks = clp // tile

    sets = max(1, bunch // row_groups)
    each = bunch // sets

    def build(step, carry):
        chunk, k = step % chunks, (step // chunks) % 3
        first = step // (3 * chunks) * bunch if spots > bunch else 0
        at = pl.multiple_of(chunk * tile, tile)
        sums = [jnp.zeros((tile, clq), f32)] * bunch
        for slot in range(slots):
            block = near[slot, k, pl.ds(at, tile), :].astype(f32)
            for place in range(bunch):
                sums[place] = sums[place] + block * weights[slot, pl.ds(first + place, 1), :]
        for part in range(sets):
            places = range(part * each, (part + 1) * each)
            wide = (first + part * each) // row_groups
            groups = [(first + place) % row_groups for place in places]
            ranks = jnp.concatenate(
                [left_turned[pl.ds(pl.multiple_of(group * clp + at, tile), tile), 0:km] for group in groups], axis=0
            )
            low = jnp.dot(
                ranks, right[k, :, pl.ds(pl.multiple_of(wide * clq, clq), clq)], preferred_element_type=f32
            )
            for number, (place, group) in enumerate(zip(places, groups)):
                dense[
                    pl.ds(pl.multiple_of(group * clp + at, tile), tile),
                    pl.ds(pl.multiple_of((wide * 3 + k) * clq, clq), clq),
                ] = (sums[place] + low[number * tile : (number + 1) * tile]).astype(bf16)
        return carry

    lax.fori_loop(0, spots // bunch * 3 * chunks, build, 0)

    @pl.when(lead == 1)
    def _():
        pl.semaphore_wait(known, n_col - 1)
        pl.semaphore_signal(known, device_id={"row": me_r - 1}, device_id_type=MESH)

    across_rows(COARSE, lambda peer: coarse_all.at[me_r], coarse_all.at[me_r])
    every(PARTS, part_codes, n_row).wait_recv()
    coarse_codes = jnp.zeros((kc, rhs), f32)
    for peer in range(n_row):
        coarse_codes = coarse_codes + part_codes[peer].astype(f32)
    coarse_codes = coarse_codes.astype(bf16)
    wave = min(row_span, 512)
    for group in range(row_span // wave):
        span = slice(group * wave, (group + 1) * wave)
        begun[span, :] = jnp.dot(left_turned[span, km:kt], coarse_codes, preferred_element_type=f32)
    pair(SLIP_NEAR, slip.at[me_r], slip.at[me_r]).wait_recv()

    def product(span, chip):
        held = jnp.concatenate([slip[pl.ds(chip * 2, 2), k].reshape(clq, rhs) for k in range(3)], axis=0)
        lanes = pl.ds(pl.multiple_of(chip * (3 * clq), 3 * clq), 3 * clq)
        return jnp.dot(dense[span, lanes], held, preferred_element_type=f32)

    for group in range(row_span // wave):
        span = slice(group * wave, (group + 1) * wave)
        begun[span, :] = begun[span, :] + product(span, own_chip)
    every(SLIP, slip, n_row - 1).wait_recv()
    for group in range(row_span // wave):
        span = slice(group * wave, (group + 1) * wave)
        value = begun[span, :]
        for step in range(1, chips):
            value = value + product(span, lax.rem(own_chip + step, chips))
        fsend[group * wave // pt : (group + 1) * wave // pt] = value.astype(bf16).reshape(
            wave // pt, pt, rhs
        )
    @pl.when(lead == 0)
    def _():
        pl.semaphore_wait(known, 1)

    across_cols(SUMS, lambda peer: fsend.at[peer], frecv.at[me_c])
    frecv[me_c] = fsend[me_c]

    every(COARSE, coarse_all, n_row).wait_recv()
    for peer in range(n_row):
        for k in range(3):
            coarse_wide[k, :, peer * pd : (peer + 1) * pd] = coarse_all[peer, k]

    def turn_over(step, carry):
        k, wide = step % 3, step // 3
        rank_turned = turn(coarse_wide[k, :, pl.ds(pl.multiple_of(wide * clq, clq), clq)]).astype(bf16)
        for group in range(row_groups):
            span = slice(group * clp, (group + 1) * clp)
            value = jnp.dot(rank_turned, left[km:kt, span], preferred_element_type=f32)
            value = value + turn(dense[span, pl.ds(pl.multiple_of(step * clq, clq), clq)])
            dense_turned[step, :, span] = value.astype(bf16)
        return carry

    lax.fori_loop(0, 3 * col_groups, turn_over, 0)

    every(SUMS, frecv, n_col).wait_recv()
    u_hat = -alpha_old[...] * u_old[...]
    for peer in range(n_col):
        u_hat = u_hat + frecv[peer].astype(f32)
    ug[me_c] = u_hat.astype(bf16)
    across_cols(LEFT, lambda peer: ug.at[me_c], ug.at[me_c])
    u_old[...] = u_hat
    every(LEFT, ug, n_col).wait_recv()

    gathered = ug[...].reshape(row_span, rhs)
    for step in range(chips):
        chip = lax.rem(own_chip + 1 + step, chips)
        for k in range(3):
            value = jnp.dot(dense_turned[chip * 3 + k], gathered, preferred_element_type=f32)
            value = value.astype(bf16).reshape(2, pd, rhs)
            for part in range(2):
                bsend[chip, part, k] = value[part]
        if step < chips - 1:
            post(BACK, {"row": chip * 2 + 1}, bsend.at[chip], brecv.at[me_r]).start()
        if step == 0:
            sq[me_r] = fold(gathered.astype(f32))
            across_rows(SQUARES, lambda peer: sq.at[me_r], sq.at[me_r])

    @pl.when(lead == 0)
    def _():
        pair(BACK, bsend.at[own_chip], brecv.at[me_r]).start()

    @pl.when(lead == 1)
    def _():
        brecv[me_r] = bsend[own_chip]

    every(SQUARES, sq, n_row).wait_recv()
    square_sum = jnp.zeros((8, rhs), f32)
    for peer in range(n_row):
        square_sum = square_sum + sq[peer]
    points = pt * n_row * n_col
    beta = jnp.sqrt(jnp.sum(square_sum, axis=0, keepdims=True) / points + tiny_add)
    beta_out[...] = beta
    inverse = 1.0 / beta
    u_out[...] = u_old[...] * inverse
    def sent():
        for place, buffer in (
            (PARTS, part_codes),
            (COARSE, coarse_all),
            (SUMS, fsend),
            (LEFT, ug),
            (SQUARES, sq),
        ):
            every(place, buffer, buffer.shape[0]).wait_send()
        every(SLIP, slip, n_row - 1).wait_send()
        pair(SLIP_NEAR, slip.at[me_r], slip.at[me_r]).wait_send()

    whole = n_row * n_col <= WHOLE_LIMIT
    leads = vsq_all.shape[0]

    @pl.when(lead == 1)
    def _():
        pair(PAIR, v_pair, v_pair).wait_recv()
        every(BACK, brecv, n_row).wait_recv()
        v_squares = jnp.zeros((8, rhs), f32)
        for part, (old, new) in enumerate([(v_pair, v_sent), (v_old, v_out)]):
            for k in range(3):
                total = jnp.zeros((pd, rhs), f32)
                for peer in range(n_row):
                    total = total + brecv[peer, part, k].astype(f32)
                v_hat = total * inverse - beta * old[k]
                new[k] = v_hat
                v_squares = v_squares + fold(v_hat)
        if whole:
            own = vsq_all.at[me_c * chips + own_chip]
            vsq_all[me_c * chips + own_chip] = jnp.sum(v_squares, axis=0, keepdims=True)
            for col in far_cols + [me_c]:
                for row in row_peers + ([] if col is me_c else [me_r]):
                    post(ALL, (row, col), own, own).start()
        else:
            vsq_col[me_c] = v_squares
            across_cols(COLS, lambda peer: vsq_col.at[me_c], vsq_col.at[me_c])
            every(COLS, vsq_col, n_col).wait_recv()
            v_squares = jnp.zeros((8, rhs), f32)
            for peer in range(n_col):
                v_squares = v_squares + vsq_col[peer]
            vsq_all[own_chip] = v_squares
            across_rows(ALL, lambda peer: vsq_all.at[own_chip], vsq_all.at[own_chip])
            every(COLS, vsq_col, n_col).wait_send()
        pair(BACK_V, v_sent, v_back).start()
        every(BACK, bsend, chips).wait_send()
        sent()
        pair(BACK_V, v_sent, v_back).wait_send()
        every(ALL, spare, spare.shape[0]).wait_send()
        every(ALL, vsq_all, leads).wait_recv()

    @pl.when(lead == 0)
    def _():
        pair(BACK_V, v_back, v_back).wait_recv()
        v_out[...] = v_back[...]
        pair(PAIR, v_old, v_pair).wait_send()
        every(BACK, bsend, chips + 1).wait_send()
        sent()
        every(ALL, vsq_all, leads + 1).wait_recv()


def finish(unknowns, u_ref, v_ref, beta_ref, squares_ref, u_out, v_out, norms_out):
    total = jnp.zeros(squares_ref.shape[1:], f32)
    for peer in range(squares_ref.shape[0]):
        total = total + squares_ref[peer]
    alpha = jnp.sqrt(jnp.sum(total, axis=0, keepdims=True) / unknowns + tiny_add)
    norms_out[0:1, :] = beta_ref[...]
    norms_out[1:2, :] = alpha
    u_out[...] = u_ref[...]
    v_out[...] = v_ref[...] / alpha


def per_device(
    n_row,
    n_col,
    u_state,
    v_state,
    alpha_prev,
    near_blocks,
    near_rows,
    near_cols,
    near_count,
    mid_left,
    mid_right,
    mid_rank,
    coarse_left,
    coarse_right,
    coarse_rank,
):
    slots, clp, _, clq = near_blocks.shape[2:]
    pt, rhs = u_state.shape
    pd = v_state.shape[1]
    km, kc = mid_left.shape[1], coarse_left.shape[1]
    kt = km + kc
    row_span, col_span = mid_left.shape[2], mid_right.shape[3]
    row_groups, col_groups = row_span // clp, col_span // clq
    in_hbm = pl.BlockSpec(memory_space=pltpu.HBM)
    vmem = pl.BlockSpec(memory_space=pltpu.VMEM)
    dma = pltpu.SemaphoreType.DMA
    whole = n_row * n_col <= WHOLE_LIMIT
    sums = (n_row // 2 * n_col, 1, rhs) if whole else (n_row // 2, 8, rhs)
    scratch = [
        pltpu.SMEM(near_rows.shape, jnp.int32),
        pltpu.SMEM(near_cols.shape, jnp.int32),
        pltpu.SMEM(near_count.shape, jnp.int32),
        pltpu.SMEM(mid_rank.shape, jnp.int32),
        pltpu.SMEM(coarse_rank.shape, jnp.int32),
        pltpu.VMEM((slots, 3, clp, clq), bf16),
        pltpu.VMEM((pt, rhs), f32),
        pltpu.VMEM((3, pd, rhs), f32),
        pltpu.VMEM((1, rhs), f32),
        pltpu.VMEM((kt, row_span), bf16),
        pltpu.VMEM((row_span, kt), bf16),
        pltpu.VMEM((3, km, col_span), bf16),
        pltpu.VMEM((n_row, 3, pd, rhs), bf16),
        pltpu.VMEM((n_row, 3, kc, pd), bf16),
        pltpu.VMEM((3, kc, col_span), bf16),
        pltpu.VMEM((row_span, rhs), f32),
        pltpu.VMEM((n_row, kc, rhs), bf16),
        pltpu.VMEM((slots, row_groups * col_groups, rhs), f32),
        pltpu.VMEM((row_span, 3 * col_span), bf16),
        pltpu.VMEM((3 * col_groups, clq, row_span), bf16),
        pltpu.VMEM((n_col, pt, rhs), bf16),
        pltpu.VMEM((n_col, pt, rhs), bf16),
        pltpu.VMEM((n_col, pt, rhs), bf16),
        pltpu.VMEM((n_row, 8, rhs), f32),
        pltpu.VMEM((n_row // 2, 2, 3, pd, rhs), bf16),
        pltpu.VMEM((n_row, 2, 3, pd, rhs), bf16),
        pltpu.VMEM((n_col, 8, rhs), f32),
        pltpu.VMEM((3, pd, rhs), f32),
        pltpu.VMEM((3, pd, rhs), f32),
        pltpu.VMEM((3, pd, rhs), f32),
        pltpu.VMEM((n_row * n_col, 1, rhs) if whole else (n_row, 8, rhs), f32),
        dma,
        dma((12,)),
        dma((12,)),
        dma((12,)),
        pltpu.SemaphoreType.REGULAR,
    ]
    held = pl.pallas_call(
        functools.partial(kernel, (n_row, n_col)),
        out_shape=(
            pltpu.VMEM((pt, rhs), f32),
            pltpu.VMEM((3, pd, rhs), f32),
            pltpu.VMEM((1, rhs), f32),
            pltpu.VMEM(sums, f32),
        ),
        in_specs=[in_hbm] * 13,
        out_specs=(vmem,) * 4,
        scratch_shapes=scratch,
        compiler_params=pltpu.CompilerParams(
            collective_id=0, has_side_effects=True, vmem_limit_bytes=60 * 1024 * 1024
        ),
        name="lsqr",
    )(
        near_rows,
        near_cols,
        near_count,
        mid_rank,
        coarse_rank,
        u_state,
        v_state,
        alpha_prev.reshape(1, rhs),
        jnp.transpose(near_blocks[0, 0], (0, 2, 1, 3)),
        mid_left[0],
        jnp.transpose(mid_right[0], (1, 0, 2)),
        coarse_left[0],
        jnp.transpose(coarse_right, (1, 0, 2)),
    )
    return pl.pallas_call(
        functools.partial(finish, 3 * pd * n_row * n_col),
        out_shape=(
            jax.ShapeDtypeStruct((pt, rhs), f32),
            jax.ShapeDtypeStruct((3, pd, rhs), f32),
            jax.ShapeDtypeStruct((2, rhs), f32),
        ),
        in_specs=[vmem] * 4,
        out_specs=(vmem,) * 3,
        name="finish",
    )(*[pltpu.with_memory_space_constraint(value, pltpu.VMEM) for value in held])


def solution(mesh):
    placed = (
        P(("row", "col"), None),
        P(None, ("col", "row"), None),
        P(),
        P("row", "col", None, None, None, None),
        P("row", "col", None),
        P("row", "col", None),
        P("row", "col"),
        P("col", None, "row"),
        P("row", None, None, "col"),
        P("row", "col"),
        P("col", None, "row"),
        P(None, None, ("col", "row")),
        P("col"),
    )
    return jax.shard_map(
        functools.partial(per_device, mesh.shape["row"], mesh.shape["col"]),
        mesh=mesh,
        in_specs=placed,
        out_specs=(P(("row", "col"), None), P(None, ("col", "row"), None), P()),
        check_vma=False,
    )
```
